32 devices in a mesh: gx: 2 (over y), gy: 4 (over z), gz: 4 (over x, core).
Axes of the slice: x: 2, y: 2, z: 4, core: 2. Of those that a mesh axis runs over, the one named last changes fastest.
Arguments:
- node_latent: bfloat16 [2, 4, 4, 512, 128], P('gx', 'gy', 'gz'), may hold values from -6 to 6
- ghost_latent: bfloat16 [2, 4, 4, 6, 64, 128], P('gx', 'gy', 'gz'), may hold values from -6 to 6
- edge_latent: bfloat16 [2, 4, 4, 2816, 128], P('gx', 'gy', 'gz'), may hold values from -6 to 6
- senders: int32 [2, 4, 4, 2816], P('gx', 'gy', 'gz'), may hold values from 0 to 895
- receivers: int32 [2, 4, 4, 2816], P('gx', 'gy', 'gz'), may hold values from 0 to 511, never falling along the last dimension, each value on 1 to 12 neighbouring positions
- export_rows: int32 [2, 4, 4, 6, 64], P('gx', 'gy', 'gz'), may hold values from 0 to 512, as said below
- node_cotangent: bfloat16 [2, 4, 4, 512, 128], P('gx', 'gy', 'gz'), may hold values from -6 to 6
- edge_cotangent: bfloat16 [2, 4, 4, 2816, 128], P('gx', 'gy', 'gz'), may hold values from -6 to 6
- w_edge_in: bfloat16 [384, 128], replicated, may hold values from -0.3125 to 0.3125
- w_edge_hidden: bfloat16 [2, 128, 128], replicated, may hold values from -0.5 to 0.5
- b_edge: float32 [3, 128], replicated, may hold values from -3 to 3
- gain_edge: float32 [128], replicated, may hold values from 0.1 to 1.9
- shift_edge: float32 [128], replicated, may hold values from -3 to 3
- w_node_in: bfloat16 [256, 128], replicated, may hold values from -0.375 to 0.375
- w_node_hidden: bfloat16 [2, 128, 128], replicated, may hold values from -0.5 to 0.5
- b_node: float32 [3, 128], replicated, may hold values from -3 to 3
- gain_node: float32 [128], replicated, may hold values from 0.1 to 1.9
Outputs:
- node_grad: float32 [2, 4, 4, 512, 128], P('gx', 'gy', 'gz')
- edge_grad: bfloat16 [2, 4, 4, 2816, 128], P('gx', 'gy', 'gz')
- grad_w_edge_in: float32 [384, 128], replicated
- grad_w_edge_hidden: float32 [2, 128, 128], replicated
- grad_b_edge: float32 [3, 128], replicated
- grad_gain_edge: float32 [128], replicated
- grad_shift_edge: float32 [128], replicated
- grad_w_node_in: float32 [256, 128], replicated
- grad_w_node_hidden: float32 [2, 128, 128], replicated
- grad_b_node: float32 [3, 128], replicated
- grad_gain_node: float32 [128], replicated
The draws below stay inside these ranges and needn't reach their ends.
Inputs may be any that keep to these rules, and one draw needn't show every extreme that they name: `export_rows`: for each block and face the leading slots hold distinct owned rows of that block; the remaining slots hold 512, marking an empty slot.
All inputs are finite; a program needn't handle non-finite values.
Results may differ from the reference program's by a relative error of at most 0.02.
Values sent between devices are 32-bit elements; how exact they have to be, the bound alone decides.
A program may use at most 64 MiB of HBM per device.

```python
import math
import jax
import jax.numpy as jnp
import numpy as np
from jax import lax

D = 128
NODES_PER_BLOCK = 512
GHOST_SLOTS = 64
EDGE_DEV = 2816
NODES = 16384
EDGES = 90112
N_GX = 2
N_GY = 4
N_GZ = 4


def draw_export_rows(key, part):
    slab_count = N_GX * N_GY * N_GZ * 6
    slab_keys = jax.random.split(jax.random.fold_in(key, 11), slab_count)

    def one_slab(slab_key):
        order_key, vacant_random_key = jax.random.split(slab_key)
        picked_slots = jax.random.permutation(order_key, NODES_PER_BLOCK)[:GHOST_SLOTS].astype(jnp.int32)
        vacant_slots = jax.random.randint(vacant_random_key, (), 0, GHOST_SLOTS // 4 + 1, dtype=jnp.int32)
        ghost_positions = jnp.arange(GHOST_SLOTS, dtype=jnp.int32)
        return jnp.where(ghost_positions < GHOST_SLOTS - vacant_slots, picked_slots, NODES_PER_BLOCK).astype(jnp.int32)
    return jax.vmap(one_slab)(slab_keys).reshape(N_GX, N_GY, N_GZ, 6, GHOST_SLOTS)


def set_ends(values, rng, low, top_value):
    longest = values.shape.index(max(values.shape))
    spots = []
    for shift in (0, 1):
        where = [jax.random.randint(jax.random.fold_in(rng, axis), (), 0, length) for axis, length in enumerate(values.shape)]
        where[longest] = (where[longest] + shift) % values.shape[longest]
        spots.append(tuple(where))
    return values.at[spots[0]].set(low).at[spots[1]].set(top_value)


def shard_levels(own_key, extent, cuts, low, largest):
    level = 1.0
    for dim, shards_of in cuts:
        draws = jax.random.uniform(jax.random.fold_in(jax.random.fold_in(own_key, 6), dim), (shards_of,), jnp.float32, low / len(cuts), largest / len(cuts))
        level = level * jnp.repeat(jnp.exp(draws), extent[dim] // shards_of).reshape((-1,) + (1,) * (len(extent) - 1 - dim))
    return level


def split_up(amount, total, limit, slope):
    portions = [(1 << 20) // math.isqrt(standing ** slope) + 1 for standing in range(2, amount + 1)]
    rest, counts = total - limit - (amount - 1), [1] * (amount - 1)
    while rest > 0:
        free = [i for i in range(amount - 1) if counts[i] < limit]
        whole, remaining = sum([portions[i] for i in free]), rest
        for i in free:
            addition = min(limit - counts[i], max(1, remaining * portions[i] // whole), rest)
            counts[i] = counts[i] + addition
            rest = rest - addition
    return np.array([limit] + counts)


def uneven_parts(stream_key, count, total, most, skew):
    if count == 2:
        one = jax.random.randint(stream_key, (), max(1, total - most), min(most, total - 1) + 1)
        return jnp.stack([one, total - one])
    lengths = jnp.asarray(split_up(count, total, most, skew), jnp.int32)
    pairs = (count - 1) // 2
    source_of, receiver = lengths[1:1 + 2 * pairs:2], lengths[2:2 + 2 * pairs:2]
    slack = jnp.minimum(source_of - 1, most - receiver)
    passed = jax.random.randint(jax.random.fold_in(stream_key, 1), (pairs,), 0, 1 << 20) % (slack + 1)
    lengths = lengths.at[1:1 + 2 * pairs:2].set(source_of - passed).at[2:2 + 2 * pairs:2].set(receiver + passed)
    return lengths[jax.random.permutation(jax.random.fold_in(stream_key, 2), count)]


def gaussian(key, dims, scale, bound, cuts=(), kind=jnp.bfloat16):
    result = jax.random.normal(key, dims, jnp.float32) * scale
    if len(cuts) > 0:
        result = shard_levels(key, dims, cuts, -0.22, 0.18) * result
    return jnp.clip(result, min=-bound, max=bound).astype(kind)


def setup_inputs(seed: int = 0) -> dict:
    key_of = jax.random.split(jax.random.key(seed), 18)
    node_latent = gaussian(key_of[0], (N_GX, N_GY, N_GZ, NODES_PER_BLOCK, D), 1.0, 6.0, ((0, 2), (1, 4), (2, 4)))
    ghost_latent = gaussian(key_of[1], (N_GX, N_GY, N_GZ, 6, GHOST_SLOTS, D), 1.0, 6.0, ((0, 2), (1, 4), (2, 4)))
    edge_latent = gaussian(key_of[2], (N_GX, N_GY, N_GZ, EDGE_DEV, D), 1.0, 6.0, ((0, 2), (1, 4), (2, 4)))
    senders = set_ends(jax.random.randint(key_of[3], (N_GX, N_GY, N_GZ, EDGE_DEV), 0, NODES_PER_BLOCK + 6 * GHOST_SLOTS), jax.random.fold_in(key_of[3], 1), 0, (NODES_PER_BLOCK + 6 * GHOST_SLOTS) - 1).astype(jnp.int32)
    receivers = jax.vmap(lambda own: jnp.searchsorted(jnp.cumsum(uneven_parts(own, NODES_PER_BLOCK, EDGE_DEV, 12, 1)), jnp.arange(EDGE_DEV), side="right"))(jax.random.split(key_of[4], N_GX * N_GY * N_GZ)).reshape((N_GX, N_GY, N_GZ, EDGE_DEV)).astype(jnp.int32)
    export_rows = draw_export_rows(jax.random.fold_in(key_of[17], 71), 0)
    node_cotangent = gaussian(key_of[6], (N_GX, N_GY, N_GZ, NODES_PER_BLOCK, D), 1.0, 6.0, ((0, 2), (1, 4), (2, 4)))
    edge_cotangent = gaussian(key_of[7], (N_GX, N_GY, N_GZ, EDGE_DEV, D), 1.0, 6.0, ((0, 2), (1, 4), (2, 4)))
    w_edge_in = gaussian(key_of[8], (3 * D, D), (3 * D) ** -0.5, 0.3125)
    w_edge_hidden = gaussian(key_of[9], (2, D, D), D ** -0.5, 0.5)
    b_edge = gaussian(key_of[10], (3, D), 0.5, 3.0, (), jnp.float32)
    gain_edge = jnp.clip(1.0 + 0.18 * jax.random.normal(key_of[11], (D,), jnp.float32), 0.1, 1.9)
    shift_edge = gaussian(key_of[12], (D,), 0.5, 3.0, (), jnp.float32)
    w_node_in = gaussian(key_of[13], (2 * D, D), (2 * D) ** -0.5, 0.375)
    w_node_hidden = gaussian(key_of[14], (2, D, D), D ** -0.5, 0.5)
    b_node = gaussian(key_of[15], (3, D), 0.5, 3.0, (), jnp.float32)
    gain_node = jnp.clip(1.0 + 0.18 * jax.random.normal(key_of[16], (D,), jnp.float32), 0.1, 1.9)
    return dict(node_latent=node_latent, ghost_latent=ghost_latent, edge_latent=edge_latent, senders=senders, receivers=receivers, export_rows=export_rows, node_cotangent=node_cotangent, edge_cotangent=edge_cotangent, w_edge_in=w_edge_in, w_edge_hidden=w_edge_hidden, b_edge=b_edge, gain_edge=gain_edge, shift_edge=shift_edge, w_node_in=w_node_in, w_node_hidden=w_node_hidden, b_node=b_node, gain_node=gain_node)


EPSILON = 1e-05

def matmul(left, right):
    return jnp.dot(left, right, preferred_element_type=jnp.float32)

def contract_rows(left, right):
    return lax.dot_general(left, right, (((0,), (0,)), ((), ())), preferred_element_type=jnp.float32)

def silu_parts(preact):
    sigmoid = jax.nn.sigmoid(preact)
    return (preact * sigmoid, sigmoid * (1.0 + preact * (1.0 - sigmoid)))

def norm_parts(preact):
    centred = preact - lax.optimization_barrier(jnp.mean(preact, -1, keepdims=True))
    inv_std = lax.rsqrt(lax.optimization_barrier(jnp.mean(centred * centred, -1, keepdims=True)) + EPSILON)
    return (centred * inv_std, inv_std)

def norm_back(grad_out, gain, normed, inv_std):
    scaled = grad_out * gain
    return inv_std * (scaled - lax.optimization_barrier(jnp.mean(scaled, -1, keepdims=True)) - normed * lax.optimization_barrier(jnp.mean(scaled * normed, -1, keepdims=True)))

def mlp_forward(inputs, w_first, w_hidden, biases):
    first_pre = matmul(inputs, w_first) + biases[0]
    first_act, first_slope = silu_parts(first_pre)
    first_out = first_act.astype(jnp.bfloat16)
    second_pre = matmul(first_out, w_hidden[0]) + biases[1]
    second_act, second_slope = silu_parts(second_pre)
    second_out = second_act.astype(jnp.bfloat16)
    final_pre = matmul(second_out, w_hidden[1]) + biases[2]
    return ((first_out, second_out, first_slope, second_slope), final_pre)

def mlp_back_inputs(final_grad, saved, w_first, w_hidden):
    first_out, second_out, first_slope, second_slope = saved
    final_round = final_grad.astype(jnp.bfloat16)
    second_grad = matmul(final_round, w_hidden[1].T) * second_slope
    second_round = second_grad.astype(jnp.bfloat16)
    first_grad = matmul(second_round, w_hidden[0].T) * first_slope
    first_round = first_grad.astype(jnp.bfloat16)
    input_grad = matmul(first_round, w_first.T)
    bias_grad = jnp.stack([lax.optimization_barrier(jnp.sum(first_grad, 0)), lax.optimization_barrier(jnp.sum(second_grad, 0)), lax.optimization_barrier(jnp.sum(final_grad, 0))])
    return ((first_round, second_round, final_round), bias_grad, input_grad)

def mlp_back_weights(inputs, saved, rounded):
    first_weight = contract_rows(inputs, rounded[0])
    hidden_weight = jnp.stack([contract_rows(saved[0], rounded[1]), contract_rows(saved[1], rounded[2])])
    return (first_weight, hidden_weight)

def forward_states(node_rows, ghost_rows, edge_rows, sender_ids, receiver_ids, params):
    node_count, feature_width = node_rows.shape
    full_rows = jnp.concatenate([node_rows, ghost_rows.reshape(-1, feature_width)], 0)
    edge_inputs = jnp.concatenate([edge_rows, full_rows[sender_ids], full_rows[receiver_ids]], 1)
    edge_stored_state, edge_pre = mlp_forward(edge_inputs, params[0], params[1], params[2])
    edge_normed, edge_inv = norm_parts(edge_pre)
    edge_new = (edge_normed * params[3] + params[4]).astype(jnp.bfloat16)
    aggregate = jax.ops.segment_sum(edge_new.astype(jnp.float32), receiver_ids, num_segments=node_count).astype(jnp.bfloat16)
    node_input_rows = jnp.concatenate([node_rows, aggregate], 1)
    node_saved, node_pre = mlp_forward(node_input_rows, params[5], params[6], params[7])
    node_normed, node_inv = norm_parts(node_pre)
    return ((edge_inputs, edge_stored_state, edge_normed, edge_inv), (node_input_rows, node_saved, node_normed, node_inv))

def node_backward(node_state, node_cot, params):
    node_input_rows, node_saved, node_normed, node_inv = node_state
    upstream = node_cot.astype(jnp.float32)
    gain_grad = lax.optimization_barrier(jnp.sum(upstream * node_normed, 0))
    final_grad = norm_back(upstream, params[8], node_normed, node_inv)
    rounded, bias_grad, input_grad = mlp_back_inputs(final_grad, node_saved, params[5], params[6])
    first_weight, hidden_weight = mlp_back_weights(node_input_rows, node_saved, rounded)
    return (input_grad, (first_weight, hidden_weight, bias_grad, gain_grad))

def edge_backward_inputs(edge_state, edge_cot, agg_grad, sender_ids, receiver_ids, total_rows, params):
    edge_inputs, edge_stored_state, edge_normed, edge_inv = edge_state
    feature_width = edge_cot.shape[1]
    edge_upstream = edge_cot.astype(jnp.float32)
    new_grad = edge_upstream + agg_grad[receiver_ids]
    gain_grad = lax.optimization_barrier(jnp.sum(new_grad * edge_normed, 0))
    shift_grad = lax.optimization_barrier(jnp.sum(new_grad, 0))
    final_grad = norm_back(new_grad, params[3], edge_normed, edge_inv)
    rounded, bias_grad, input_grad = mlp_back_inputs(final_grad, edge_stored_state, params[0], params[1])
    edge_grad = (edge_upstream + input_grad[:, :feature_width]).astype(jnp.bfloat16)
    full_grad = jax.ops.segment_sum(input_grad[:, feature_width:2 * feature_width], sender_ids, num_segments=total_rows)
    full_grad = full_grad + jax.ops.segment_sum(input_grad[:, 2 * feature_width:], receiver_ids, num_segments=total_rows)
    return (edge_grad, full_grad, rounded, (bias_grad, gain_grad, shift_grad))

def block_pass(node_rows, ghost_rows, edge_rows, sender_ids, receiver_ids, node_cot, edge_cot, params):
    node_count, feature_width = node_rows.shape
    total_rows = node_count + ghost_rows.shape[0] * ghost_rows.shape[1]
    edge_state, node_state = forward_states(node_rows, ghost_rows, edge_rows, sender_ids, receiver_ids, params)
    node_input_grad, node_weights = node_backward(node_state, node_cot, params)
    edge_grad, full_grad, rounded, edge_small = edge_backward_inputs(edge_state, edge_cot, node_input_grad[:, feature_width:], sender_ids, receiver_ids, total_rows, params)
    first_weight, hidden_weight = mlp_back_weights(edge_state[0], edge_state[1], rounded)
    local_grad = node_cot.astype(jnp.float32) + node_input_grad[:, :feature_width] + full_grad[:node_count]
    ghost_grad = full_grad[node_count:].reshape(ghost_rows.shape)
    weights = (first_weight, hidden_weight) + edge_small + node_weights
    return (local_grad, ghost_grad, edge_grad, weights)

def add_rows(target, rows, values):
    return target.at[rows].add(values, mode='drop')

def reference(node_latent, ghost_latent, edge_latent, senders, receivers, export_rows, node_cotangent, edge_cotangent, w_edge_in, w_edge_hidden, b_edge, gain_edge, shift_edge, w_node_in, w_node_hidden, b_node, gain_node):
    params = (w_edge_in, w_edge_hidden, b_edge, gain_edge, shift_edge, w_node_in, w_node_hidden, b_node, gain_node)
    block_count = N_GX * N_GY * N_GZ
    grid_shape = (N_GX, N_GY, N_GZ)

    def flatten(array):
        return array.reshape((block_count,) + array.shape[3:])
    stacked = tuple((flatten(array) for array in (node_latent, ghost_latent, edge_latent, senders, receivers, node_cotangent, edge_cotangent)))

    def visit(running, block_item):
        local_grad, ghost_grad, edge_grad, weights = block_pass(*block_item, params)
        return (tuple((total + term for total, term in zip(running, weights))), (local_grad, ghost_grad, edge_grad))
    start = tuple((jnp.zeros(param.shape, jnp.float32) for param in params))
    totals, (local_all, ghost_all, edge_all) = lax.scan(visit, start, stacked)
    ghost_grid = ghost_all.reshape(grid_shape + ghost_all.shape[1:])
    rows_flat = flatten(export_rows)
    node_grad = local_all
    for face_index in range(6):
        incoming = jnp.roll(ghost_grid[:, :, :, face_index], 1 - 2 * (face_index % 2), face_index // 2)
        node_grad = jax.vmap(add_rows)(node_grad, rows_flat[:, face_index], flatten(incoming))
    node_grad = node_grad.reshape(grid_shape + node_grad.shape[1:])
    edge_grad = edge_all.reshape(grid_shape + edge_all.shape[1:])
    edge_scale = EDGES ** (-0.5)
    node_scale = NODES ** (-0.5)
    return (node_grad, edge_grad, totals[0] * edge_scale, totals[1] * edge_scale, totals[2] * edge_scale, totals[3] * edge_scale, totals[4] * edge_scale, totals[5] * node_scale, totals[6] * node_scale, totals[7] * node_scale, totals[8] * node_scale)
```

```python
import functools

import jax
import jax.numpy as jnp
from jax import lax
from jax.experimental import pallas as pl
from jax.experimental.pallas import tpu as pltpu
from jax.sharding import PartitionSpec as P

EPSILON = 1e-05
LANES = 128
FORWARD_TILE = 512
BACKWARD_TILE = 512
MESH = pl.DeviceIdType.MESH
AXES = ("gx", "gy", "gz")


def matmul(left, right):
    return jnp.dot(left, right, preferred_element_type=jnp.float32)


def matmul_nt(left, right):
    return lax.dot_general(
        left, right, (((1,), (1,)), ((), ())), preferred_element_type=jnp.float32
    )


def contract_rows(left, right):
    return lax.dot_general(
        left, right, (((0,), (0,)), ((), ())), preferred_element_type=jnp.float32
    )


def silu_parts(half):
    th = jnp.tanh(half)
    lifted = 1.0 + th
    act = half * lifted
    return act, lifted + act * (1.0 - th)


def norm_parts(preact):
    centred = preact - jnp.mean(preact, 0, keepdims=True)
    inv_std = lax.rsqrt(jnp.mean(centred * centred, 0, keepdims=True) + EPSILON)
    return centred * inv_std, inv_std


def norm_back(scaled, normed, inv_std):
    return inv_std * (
        scaled
        - jnp.mean(scaled, 0, keepdims=True)
        - normed * jnp.mean(scaled * normed, 0, keepdims=True)
    )


def rows_sum(values):
    return jnp.sum(values, 0, keepdims=True)


def one_hot(hit):
    return jnp.where(hit, 1.0, 0.0).astype(jnp.bfloat16)


def wide(column, lanes):
    return jnp.concatenate([column] * (lanes // LANES), 1)


def lane_fold(values):
    total = values[:, :LANES]
    for start in range(LANES, values.shape[1], LANES):
        total = total + values[:, start : start + LANES]
    return total


def chain(lefts, rights):
    total = None
    for start in range(0, len(lefts), 2):
        left = jnp.concatenate(lefts[start : start + 2], 1)
        right = jnp.concatenate(rights[start : start + 2], 0)
        term = matmul(left, right)
        total = term if total is None else total + term
    return total


def stage_groups(sizes):
    near = [("gx", sizes["gx"], 1), ("gz", sizes["gz"], 1)]
    far = [("gy", sizes["gy"], 1)]
    return near, far


def group_size(group):
    count = 1
    for _, members, _ in group:
        count *= members
    return count


def coordinate(part):
    axis, count, stride = part
    return lax.rem(lax.axis_index(axis) // stride, count)


def member(group):
    index = 0
    for part in group:
        index = index * part[1] + coordinate(part)
    return index


def peers(group):
    steps = [()]
    for part in group:
        steps = [step + (more,) for step in steps for more in range(part[1])]
    found = []
    for step in steps[1:]:
        index = 0
        device = {}
        for part, more in zip(group, step):
            axis, count, stride = part
            mine = coordinate(part)
            other = lax.rem(mine + more, count)
            index = index * count + other
            here = device.get(axis, lax.axis_index(axis))
            device[axis] = here + (other - mine) * stride
        found.append((index, device))
    return found


class Reducer:
    def __init__(self, first, second, source, out, scratch):
        self.first, self.second = first, second
        self.source, self.out = source, out
        self.landing, self.swap, self.part = scratch[:3]
        self.sems = scratch[3:]
        self.piece = source.shape[0] // group_size(first)
        self.home = pl.ds(pl.multiple_of(member(first) * self.piece, 8), self.piece)
        self.pending = []

    def send(self, source, target, device, spot, stage):
        copy = pltpu.make_async_remote_copy(
            src_ref=source,
            dst_ref=target,
            send_sem=self.sems[2 * stage].at[spot],
            recv_sem=self.sems[2 * stage + 1].at[spot],
            device_id=device,
            device_id_type=MESH,
        )
        copy.start()
        self.pending.append(copy)

    def wait(self):
        for copy in self.pending:
            copy.wait()
        self.pending = []

    def scatter(self):
        for spot, (other, device) in enumerate(peers(self.first)):
            rows = pl.ds(pl.multiple_of(other * self.piece, 8), self.piece)
            self.send(self.source.at[rows], self.landing.at[spot], device, spot, 0)

    def exchange(self):
        self.wait()
        total = self.source[self.home]
        for spot in range(group_size(self.first) - 1):
            total = total + self.landing[spot]
        mine = member(self.second)
        self.part[...] = total
        self.swap[mine] = total
        for spot, (_, device) in enumerate(peers(self.second)):
            self.send(self.part, self.swap.at[mine], device, spot, 1)

    def gather(self):
        self.wait()
        total = self.swap[0]
        for index in range(1, group_size(self.second)):
            total = total + self.swap[index]
        self.out[self.home] = total
        for spot, (_, device) in enumerate(peers(self.first)):
            self.send(self.out.at[self.home], self.out.at[self.home], device, spot, 2)


def reducer_scratch(first, second, rows, width):
    one, two = group_size(first), group_size(second)
    piece = rows // one
    dma = pltpu.SemaphoreType.DMA
    return [
        pltpu.VMEM((one - 1, piece, width), jnp.float32),
        pltpu.VMEM((two, piece, width), jnp.float32),
        pltpu.VMEM((piece, width), jnp.float32),
        dma((one - 1,)),
        dma((one - 1,)),
        dma((two - 1,)),
        dma((two - 1,)),
        dma((one - 1,)),
        dma((one - 1,)),
    ]


def tiles(rows, size):
    return [(start, min(size, rows - start)) for start in range(0, rows, size)]


def face_target(sizes, face):
    axis, side = AXES[face // 2], face % 2
    count = sizes[axis]
    step = 1 if side == 0 else count - 1
    return {axis: lax.rem(lax.axis_index(axis) + step, count)}


def block_kernel(
    sizes,
    edge_scale,
    node_scale,
    node,
    ghost,
    edge,
    snd,
    rcv,
    faces,
    ncot,
    ecot,
    we1,
    weh,
    be,
    ge,
    se,
    wn1,
    wnh,
    bn,
    gn,
    node_o,
    edge_o,
    nred_o,
    ared_o,
    bred_o,
    node_id,
    snd_col,
    rcv_col,
    table,
    z1_s,
    z2_s,
    r1_s,
    slope1_s,
    slope2_s,
    normed_s,
    inv_s,
    npack,
    apack,
    bpack,
    edge_s,
    ecot_s,
    ghost_s,
    halo,
    loads,
    hsend,
    hland,
    *scratch,
):
    nodes, width = node.shape
    edges = edge.shape[0]
    ghosts = ghost.shape[0]
    slots = ghosts // 6
    total = nodes + ghosts
    bf16, f32 = jnp.bfloat16, jnp.float32
    near, far = stage_groups(sizes)
    third = len(scratch) // 3
    node_red = Reducer(near, far, npack, nred_o, scratch[:third])
    a_red = Reducer(near, far, apack, ared_o, scratch[third : 2 * third])
    b_red = Reducer(far, near, bpack, bred_o, scratch[2 * third :])

    loaded = [
        pltpu.make_async_copy(edge, edge_s, loads.at[0]),
        pltpu.make_async_copy(ecot, ecot_s, loads.at[1]),
    ]
    for copy in loaded:
        copy.start()
    barrier = pltpu.get_barrier_semaphore()
    greeted = [face_target(sizes, face) for face in range(6)]
    for group in (near, far):
        greeted += [device for _, device in peers(group)]
    for device in greeted:
        pl.semaphore_signal(barrier, inc=1, device_id=device, device_id_type=MESH)

    lane = lax.broadcasted_iota(jnp.int32, (LANES, LANES), 1).astype(jnp.int16)
    sub = lax.broadcasted_iota(jnp.int32, (LANES, LANES), 0)
    one = jnp.ones((LANES, LANES), bf16)
    zero = jnp.zeros((LANES, LANES), bf16)
    for part in range(total // LANES):
        node_id[part] = (sub + part * LANES).astype(jnp.int16)

    def column(row):
        return jnp.transpose(jnp.broadcast_to(row, (LANES, LANES)))

    for block in range(edges // LANES):
        at = slice(block * LANES, (block + 1) * LANES)
        snd_col[block] = column(snd[:, at]).astype(jnp.int16)
        rcv_col[block] = column(rcv[:, at]).astype(jnp.int16)

    def node_hots(ids, start, size, count):
        rows = [
            jnp.broadcast_to(ids[:, spot : spot + LANES], (LANES, LANES)).astype(jnp.int16)
            for spot in range(start, start + size, LANES)
        ]
        return [
            jnp.concatenate([jnp.where(row == node_id[part], one, zero) for row in rows], 1)
            for part in range(count // LANES)
        ]

    def edge_hots(columns, block, first, count):
        ids = columns[block]
        return jnp.concatenate(
            [
                jnp.where(ids == lane + jnp.int16(part * LANES), one, zero)
                for part in range(first // LANES, (first + count) // LANES)
            ],
            1,
        )

    def blocks_of(ref, start, size):
        spots = range(start // LANES, (start + size) // LANES)
        return jnp.concatenate([ref[spot] for spot in spots], 1)

    def put_blocks(ref, start, values):
        for spot in range(values.shape[1] // LANES):
            ref[start // LANES + spot] = values[:, spot * LANES : (spot + 1) * LANES]

    half = jnp.bfloat16(0.5)
    half_t = lambda weight: jnp.transpose(weight * half)
    w1 = [half_t(we1[index * width : (index + 1) * width]) for index in range(3)]
    w2, w3 = half_t(weh[0]), jnp.transpose(weh[1])
    back3, back2 = weh[1] * half, weh[0] * half
    bias = [column(0.5 * be[0:1]), column(0.5 * be[1:2]), column(be[2:3])]
    gain, shift = column(ge[...]), column(se[...])

    put_blocks(table, 0, matmul_nt(w1[1], node[...]).astype(bf16))
    put_blocks(table, nodes, matmul_nt(w1[1], ghost[...]).astype(bf16))
    put_blocks(table, total, matmul_nt(w1[2], node[...]).astype(bf16))
    spots = (total + nodes) // LANES

    loaded[0].wait()
    agg = None
    for start, size in tiles(edges, FORWARD_TILE):
        at = pl.ds(start, size)
        rights = [jnp.transpose(edge_s[at])]
        rights += node_hots(snd, start, size, total) + node_hots(rcv, start, size, nodes)
        first = chain([w1[0]] + [table[spot] for spot in range(spots)], rights)
        act, slope = silu_parts(first + wide(bias[0], size))
        z1 = act.astype(bf16)
        put_blocks(z1_s, start, z1)
        put_blocks(slope1_s, start, slope)
        act, slope = silu_parts(matmul(w2, z1) + wide(bias[1], size))
        z2 = act.astype(bf16)
        put_blocks(z2_s, start, z2)
        put_blocks(slope2_s, start, slope)
        normed, inv = norm_parts(matmul(w3, z2) + wide(bias[2], size))
        put_blocks(normed_s, start, normed)
        put_blocks(inv_s, start, inv)
        new = (normed * wide(gain, size) + wide(shift, size)).astype(bf16)
        lefts = [new[:, spot : spot + LANES] for spot in range(0, size, LANES)]
        rights = [edge_hots(rcv_col, (start + spot) // LANES, 0, nodes) for spot in range(0, size, LANES)]
        term = chain(lefts, rights)
        agg = term if agg is None else agg + term

    agg = agg.astype(bf16)
    n1a, n1b = half_t(wn1[:width]), half_t(wn1[width:])
    n2, n3 = half_t(wnh[0]), jnp.transpose(wnh[1])
    first = matmul_nt(n1a, node[...]) + matmul(n1b, agg)
    act, slope1 = silu_parts(first + wide(column(0.5 * bn[0:1]), nodes))
    z1 = act.astype(bf16)
    act, slope2 = silu_parts(matmul(n2, z1) + wide(column(0.5 * bn[1:2]), nodes))
    z2 = act.astype(bf16)
    normed, inv = norm_parts(matmul(n3, z2) + wide(column(bn[2:3]), nodes))
    up = jnp.transpose(ncot[...]).astype(f32)
    gain_sum = lane_fold(up * normed)
    g3 = norm_back(up * wide(column(gn[...]), nodes), normed, inv)
    r3 = g3.astype(bf16)
    g2 = matmul(wnh[1] * half, r3) * slope2
    r2 = g2.astype(bf16)
    g1 = matmul(wnh[0] * half, r2) * slope1
    r1 = g1.astype(bf16)
    agg_grad = matmul(wn1[width:], r1).astype(bf16)
    node_part = up + matmul(wn1[:width], r1)
    node_terms = [jnp.transpose(matmul(r1, node[...])), matmul_nt(agg, r1)]
    node_terms += [matmul_nt(z1, r2), matmul_nt(z2, r3)]
    for index, term in enumerate(node_terms):
        npack[index * width : (index + 1) * width] = term * node_scale
    for pack, used in ((npack, 4 * width), (apack, 4 * width), (bpack, width)):
        if pack.shape[0] > used:
            pack[used:] = jnp.zeros((pack.shape[0] - used, width), f32)

    def row_of(folded):
        return rows_sum(jnp.transpose(folded))

    node_sums = (lane_fold(g1), lane_fold(g2), lane_fold(g3), gain_sum)
    for index, value in enumerate(node_sums):
        bpack[width + 5 + index : width + 6 + index] = row_of(value) * node_scale

    pl.semaphore_wait(barrier, len(greeted))
    node_red.scatter()

    loaded[1].wait()
    small = [None] * 5
    grads = [None] * 3
    more = lambda old, new: new if old is None else old + new
    lefts = [agg_grad[:, spot : spot + LANES] for spot in range(0, nodes, LANES)]
    for start, size in tiles(edges, BACKWARD_TILE):
        at = pl.ds(start, size)
        up = jnp.transpose(ecot_s[at]).astype(f32)
        up = up + chain(lefts, node_hots(rcv, start, size, nodes))
        normed = blocks_of(normed_s, start, size)
        g3 = norm_back(up * wide(gain, size), normed, blocks_of(inv_s, start, size))
        r3 = g3.astype(bf16)
        g2 = matmul(back3, r3) * blocks_of(slope2_s, start, size)
        r2 = g2.astype(bf16)
        g1 = matmul(back2, r2) * blocks_of(slope1_s, start, size)
        r1 = g1.astype(bf16)
        put_blocks(r1_s, start, r1)
        grads[0] = more(grads[0], matmul(r1, edge_s[at]))
        grads[1] = more(grads[1], matmul_nt(blocks_of(z1_s, start, size), r2))
        grads[2] = more(grads[2], matmul_nt(blocks_of(z2_s, start, size), r3))
        for index, term in enumerate((g1, g2, g3, up * normed, up)):
            small[index] = more(small[index], lane_fold(term))

    lefts = [r1_s[block] for block in range(edges // LANES)]
    by_sender = []
    for start, size in tiles(total, 2 * LANES):
        rights = [edge_hots(snd_col, block, start, size) for block in range(edges // LANES)]
        by_sender.append(chain(lefts, rights).astype(bf16))
    by_receiver = []
    for start, size in tiles(nodes, 2 * LANES):
        rights = [edge_hots(rcv_col, block, start, size) for block in range(edges // LANES)]
        by_receiver.append(chain(lefts, rights).astype(bf16))
    by_sender = jnp.concatenate(by_sender, 1)
    by_receiver = jnp.concatenate(by_receiver, 1)
    middle = matmul(by_sender[:, :nodes], node[...]) + matmul(by_sender[:, nodes:], ghost[...])
    last = matmul(by_receiver, node[...])
    turned = [jnp.transpose(term) for term in (grads[0], middle, last)]
    for index, term in enumerate(turned + [grads[1]]):
        apack[index * width : (index + 1) * width] = term * edge_scale
    bpack[:width] = grads[2] * edge_scale
    for index, value in enumerate(small):
        bpack[width + index : width + 1 + index] = row_of(value) * edge_scale
    a_red.scatter()
    b_red.scatter()
    node_red.exchange()

    full = matmul(we1[width : 2 * width], by_sender)
    ghost_s[...] = jnp.transpose(full[:, nodes:])
    halos = []
    for face in range(6):
        rows = pl.ds(face * slots, slots)
        copy = pltpu.make_async_remote_copy(
            src_ref=ghost_s.at[rows],
            dst_ref=halo.at[rows],
            send_sem=hsend.at[face],
            recv_sem=hland.at[face],
            device_id=face_target(sizes, face),
            device_id_type=MESH,
        )
        copy.start()
        halos.append(copy)
    node_part = node_part + full[:, :nodes] + matmul(we1[2 * width :], by_receiver)
    node_o[...] = jnp.transpose(node_part)

    def edge_out(first, last):
        for block in range(first, last):
            at = pl.ds(block * LANES, LANES)
            grad = ecot_s[at].astype(f32) + matmul_nt(jnp.transpose(r1_s[block]), we1[:width])
            edge_o[at] = grad.astype(bf16)

    middle_block = edges // LANES // 2
    edge_out(0, middle_block)
    a_red.exchange()
    b_red.exchange()
    node_red.gather()
    edge_out(middle_block, edges // LANES)
    for copy in halos:
        copy.wait()
    spot = lax.broadcasted_iota(jnp.int32, (nodes, slots), 0)
    local = node_o[...]
    for face in range(6):
        values = halo[face * slots : (face + 1) * slots].astype(bf16)
        local = local + matmul(one_hot(spot == faces[face]), values)
    node_o[...] = local
    a_red.gather()
    b_red.gather()
    node_red.wait()
    a_red.wait()
    b_red.wait()


def finish_kernel(
    node, edge, nred, ared, bred, node_o, edge_o, we1_o, weh_o, be_o, ge_o, se_o, wn1_o, wnh_o, bn_o, gn_o
):
    width = node.shape[1]
    node_o[...] = node[...]
    edge_o[...] = edge[...]
    we1_o[...] = ared[: 3 * width]
    weh_o[0] = ared[3 * width : 4 * width]
    weh_o[1] = bred[:width]
    wn1_o[...] = nred[: 2 * width]
    wnh_o[0] = nred[2 * width : 3 * width]
    wnh_o[1] = nred[3 * width : 4 * width]
    be_o[...] = bred[width : width + 3]
    ge_o[...] = bred[width + 3 : width + 4]
    se_o[...] = bred[width + 4 : width + 5]
    bn_o[...] = bred[width + 5 : width + 8]
    gn_o[...] = bred[width + 8 : width + 9]


VMEM = pl.BlockSpec(memory_space=pltpu.VMEM)
HBM = pl.BlockSpec(memory_space=pl.ANY)


def on_device(
    sizes,
    node_latent,
    ghost_latent,
    edge_latent,
    senders,
    receivers,
    export_rows,
    node_cotangent,
    edge_cotangent,
    w_edge_in,
    w_edge_hidden,
    b_edge,
    gain_edge,
    shift_edge,
    w_node_in,
    w_node_hidden,
    b_node,
    gain_node,
):
    f32, bf16 = jnp.float32, jnp.bfloat16
    nodes, width = node_latent.shape[3:]
    slots = ghost_latent.shape[4]
    ghosts = 6 * slots
    edges = edge_latent.shape[3]
    total = nodes + ghosts
    devices = sizes["gx"] * sizes["gy"] * sizes["gz"]
    edge_scale = float(edges * devices) ** (-0.5)
    node_scale = float(nodes * devices) ** (-0.5)

    def padded(rows, group):
        unit = 8 * group_size(group)
        return -(-rows // unit) * unit

    def shape(*dims, dtype=f32):
        return jax.ShapeDtypeStruct(dims, dtype)

    near, far = stage_groups(sizes)
    four, two = padded(4 * width, near), padded(width + 9, far)
    reducers = reducer_scratch(near, far, four, width)
    reducers += reducer_scratch(near, far, four, width)
    reducers += reducer_scratch(far, near, two, width)
    passed = pl.pallas_call(
        functools.partial(block_kernel, sizes, edge_scale, node_scale),
        out_shape=(
            shape(nodes, width),
            shape(edges, width, dtype=bf16),
            shape(four, width),
            shape(four, width),
            shape(two, width),
        ),
        in_specs=[VMEM] * 2 + [HBM] + [VMEM] * 4 + [HBM] + [VMEM] * 9,
        out_specs=(VMEM,) * 5,
        scratch_shapes=[
            pltpu.VMEM((total // LANES, LANES, LANES), jnp.int16),
            pltpu.VMEM((edges // LANES, LANES, LANES), jnp.int16),
            pltpu.VMEM((edges // LANES, LANES, LANES), jnp.int16),
            pltpu.VMEM(((total + nodes) // LANES, LANES, LANES), bf16),
            pltpu.VMEM((edges // LANES, LANES, LANES), bf16),
            pltpu.VMEM((edges // LANES, LANES, LANES), bf16),
            pltpu.VMEM((edges // LANES, LANES, LANES), bf16),
            pltpu.VMEM((edges // LANES, LANES, LANES), f32),
            pltpu.VMEM((edges // LANES, LANES, LANES), f32),
            pltpu.VMEM((edges // LANES, LANES, LANES), f32),
            pltpu.VMEM((edges // LANES, 1, LANES), f32),
            pltpu.VMEM((four, width), f32),
            pltpu.VMEM((four, width), f32),
            pltpu.VMEM((two, width), f32),
            pltpu.VMEM((edges, width), bf16),
            pltpu.VMEM((edges, width), bf16),
            pltpu.VMEM((ghosts, width), f32),
            pltpu.VMEM((ghosts, width), f32),
            pltpu.SemaphoreType.DMA((2,)),
            pltpu.SemaphoreType.DMA((6,)),
            pltpu.SemaphoreType.DMA((6,)),
        ]
        + reducers,
        compiler_params=pltpu.CompilerParams(
            collective_id=0, has_side_effects=True, vmem_limit_bytes=60 * 1024 * 1024
        ),
        name="block_pass",
    )(
        node_latent.reshape(nodes, width),
        ghost_latent.reshape(ghosts, width),
        edge_latent.reshape(edges, width),
        senders.reshape(1, edges),
        receivers.reshape(1, edges),
        export_rows.reshape(6, 1, slots),
        node_cotangent.reshape(nodes, width),
        edge_cotangent.reshape(edges, width),
        w_edge_in,
        w_edge_hidden,
        b_edge,
        gain_edge.reshape(1, width),
        shift_edge.reshape(1, width),
        w_node_in,
        w_node_hidden,
        b_node,
        gain_node.reshape(1, width),
    )

    outs = pl.pallas_call(
        finish_kernel,
        out_shape=(
            shape(nodes, width),
            shape(edges, width, dtype=bf16),
            shape(3 * width, width),
            shape(2, width, width),
            shape(3, width),
            shape(1, width),
            shape(1, width),
            shape(2 * width, width),
            shape(2, width, width),
            shape(3, width),
            shape(1, width),
        ),
        in_specs=[VMEM] * 5,
        out_specs=(VMEM,) * 11,
        name="finish",
    )(*passed)
    node_grad, edge_grad, we1, weh, be, ge, se, wn1, wnh, bn, gn = outs
    return (
        node_grad.reshape(node_latent.shape),
        edge_grad.reshape(edge_latent.shape),
        we1,
        weh,
        be,
        ge.reshape(width),
        se.reshape(width),
        wn1,
        wnh,
        bn,
        gn.reshape(width),
    )


def solution(mesh):
    block = P("gx", "gy", "gz")
    sizes = dict(mesh.shape)
    return jax.shard_map(
        functools.partial(on_device, sizes),
        mesh=mesh,
        in_specs=(block,) * 8 + (P(),) * 9,
        out_specs=(block,) * 2 + (P(),) * 9,
        check_vma=False,
    )
```

```python
import functools

import jax
import jax.numpy as jnp
from jax import lax
from jax.experimental import pallas as pl
from jax.experimental.pallas import tpu as pltpu
from jax.sharding import PartitionSpec as P

EPSILON = 1e-05
LANES = 128
FORWARD_TILE = 1408
BACKWARD_TILE = 1408
MESH = pl.DeviceIdType.MESH
AXES = ("gx", "gy", "gz")


def matmul(left, right):
    return jnp.dot(left, right, preferred_element_type=jnp.float32)


def matmul_nt(left, right):
    return lax.dot_general(
        left, right, (((1,), (1,)), ((), ())), preferred_element_type=jnp.float32
    )


def contract_rows(left, right):
    return lax.dot_general(
        left, right, (((0,), (0,)), ((), ())), preferred_element_type=jnp.float32
    )


def silu_parts(half):
    th = jnp.tanh(half)
    lifted = 1.0 + th
    act = half * lifted
    return act, lifted + act * (1.0 - th)


def norm_parts(preact):
    centred = preact - jnp.mean(preact, 0, keepdims=True)
    inv_std = lax.rsqrt(jnp.mean(centred * centred, 0, keepdims=True) + EPSILON)
    return centred * inv_std, inv_std


def norm_back(scaled, normed, inv_std):
    return inv_std * (
        scaled
        - jnp.mean(scaled, 0, keepdims=True)
        - normed * jnp.mean(scaled * normed, 0, keepdims=True)
    )


def rows_sum(values):
    return jnp.sum(values, 0, keepdims=True)


def one_hot(hit):
    return jnp.where(hit, 1.0, 0.0).astype(jnp.bfloat16)


def wide(column, lanes):
    return jnp.concatenate([column] * (lanes // LANES), 1)


def lane_fold(values):
    total = values[:, :LANES]
    for start in range(LANES, values.shape[1], LANES):
        total = total + values[:, start : start + LANES]
    return total


def chain(lefts, rights):
    total = None
    for start in range(0, len(lefts), 2):
        left = jnp.concatenate(lefts[start : start + 2], 1)
        right = jnp.concatenate(rights[start : start + 2], 0)
        term = matmul(left, right)
        total = term if total is None else total + term
    return total


def stage_groups(sizes):
    pair = 2 if sizes["gz"] % 2 == 0 else 1
    core = [("gz", pair, 1)]
    chips = [("gx", sizes["gx"], 1), ("gz", sizes["gz"] // pair, pair)]
    near = [("gx", sizes["gx"], 1), ("gz", sizes["gz"], 1)]
    far = [("gy", sizes["gy"], 1)]
    return core, chips, near, far


def group_size(group):
    count = 1
    for _, members, _ in group:
        count *= members
    return count


def coordinate(part):
    axis, count, stride = part
    return lax.rem(lax.axis_index(axis) // stride, count)


def member(group):
    index = 0
    for part in group:
        index = index * part[1] + coordinate(part)
    return index


def peers(group):
    steps = [()]
    for part in group:
        steps = [step + (more,) for step in steps for more in range(part[1])]
    found = []
    for step in steps[1:]:
        index = 0
        device = {}
        for part, more in zip(group, step):
            axis, count, stride = part
            mine = coordinate(part)
            other = lax.rem(mine + more, count)
            index = index * count + other
            here = device.get(axis, lax.axis_index(axis))
            device[axis] = here + (other - mine) * stride
        found.append((index, device))
    return found


class Reducer:
    def __init__(self, groups, last, source, out, scratch):
        self.groups, self.last, self.source, self.out = groups, last, source, out
        self.scratch = list(scratch)
        self.now, self.spot, self.rows = source, 0, source.shape[0]
        self.homes = []
        self.pending = []
        self.steps = [functools.partial(self.scatter, group) for group in groups]
        self.steps += [self.exchange, self.settle]
        self.steps += [functools.partial(self.gather, group) for group in groups[-2::-1]]
        self.steps += [self.wait]

    def advance(self):
        self.steps.pop(0)()

    def send(self, source, target, device, spot, sems):
        copy = pltpu.make_async_remote_copy(
            src_ref=source,
            dst_ref=target,
            send_sem=sems[0].at[spot],
            recv_sem=sems[1].at[spot],
            device_id=device,
            device_id_type=MESH,
        )
        copy.start()
        self.pending.append(copy)

    def wait(self):
        for copy in self.pending:
            copy.wait()
        self.pending = []

    def fold(self):
        if not self.homes:
            return
        self.wait()
        landing, part, own = self.arrived
        total = own[...]
        for spot in range(self.count):
            total = total + landing[spot]
        part[...] = total
        self.now = part

    def scatter(self, group):
        self.fold()
        landing, part, *sems = self.scratch[:4]
        self.scratch = self.scratch[4:]
        piece = self.now.shape[0] // group_size(group)
        for spot, (other, device) in enumerate(peers(group)):
            rows = pl.ds(pl.multiple_of(other * piece, 8), piece)
            self.send(self.now.at[rows], landing.at[spot], device, spot, sems)
        self.count = group_size(group) - 1
        mine = member(group) * piece
        self.spot = self.spot + mine
        self.homes.append((self.spot, piece))
        self.arrived = landing, part, self.now.at[pl.ds(pl.multiple_of(mine, 8), piece)]

    def exchange(self):
        self.fold()
        swap, *sems = self.scratch[:3]
        self.scratch = self.scratch[3:]
        mine = member(self.last)
        swap[mine] = self.now[...]
        for spot, (_, device) in enumerate(peers(self.last)):
            self.send(self.now, swap.at[mine], device, spot, sems)
        self.swap = swap

    def settle(self):
        self.wait()
        total = self.swap[0]
        for index in range(1, group_size(self.last)):
            total = total + self.swap[index]
        start, piece = self.homes[-1]
        self.out[pl.ds(pl.multiple_of(start, 8), piece)] = total
        self.gather(self.groups[-1])

    def gather(self, group):
        self.wait()
        start, piece = self.homes.pop()
        sems = self.scratch[:2]
        self.scratch = self.scratch[2:]
        home = self.out.at[pl.ds(pl.multiple_of(start, 8), piece)]
        for spot, (_, device) in enumerate(peers(group)):
            self.send(home, home, device, spot, sems)


def reducer_scratch(groups, last, rows, width):
    dma = pltpu.SemaphoreType.DMA
    found = []
    for group in groups:
        count = group_size(group)
        rows = rows // count
        found += [pltpu.VMEM((max(count - 1, 1), rows, width), jnp.float32)]
        found += [pltpu.VMEM((rows, width), jnp.float32)]
        found += [dma((max(count - 1, 1),))] * 2
    count = group_size(last)
    found += [pltpu.VMEM((count, rows, width), jnp.float32)] + [dma((max(count - 1, 1),))] * 2
    for group in groups[::-1]:
        found += [dma((max(group_size(group) - 1, 1),))] * 2
    return found


def tiles(rows, size):
    return [(start, min(size, rows - start)) for start in range(0, rows, size)]


def face_target(sizes, face):
    axis, side = AXES[face // 2], face % 2
    count = sizes[axis]
    step = 1 if side == 0 else count - 1
    return {axis: lax.rem(lax.axis_index(axis) + step, count)}


INPUTS = 17


def block_kernel(sizes, edge_scale, node_scale, counts, *refs):
    refs = list(refs)
    take = lambda count: [refs.pop(0) for _ in range(count)]
    sources = take(INPUTS)
    node_o, edge_o, nred_o, bred_o, ared_o, be_o, ge_o, se_o, bn_o, gn_o = take(10)
    held = take(INPUTS)
    node, ghost, edge, snd, rcv, faces, ncot, ecot, we1, weh, be, ge, se, wn1, wnh, bn, gn = held
    node_id, lane_id, snd_col, rcv_col, table, z1_s, z2_s, r1_s, slope1_s, slope2_s, normed_s, inv_s = take(12)
    npack, bpack, apack, ghost_s, halo, loads, hsend, hland = take(8)
    scratch = [take(count) for count in counts]
    nodes, width = node.shape
    edges = edge.shape[0]
    ghosts = ghost.shape[0]
    slots = ghosts // 6
    total = nodes + ghosts
    bf16, f32 = jnp.bfloat16, jnp.float32
    core, chips, near, far = stage_groups(sizes)
    node_red = Reducer([core, chips], far, npack, nred_o, scratch[0])
    b_red = Reducer([near], far, bpack, bred_o, scratch[1])
    a_red = Reducer([near], far, apack, ared_o, scratch[2])

    loaded = [
        pltpu.make_async_copy(source, target, loads.at[index])
        for index, (source, target) in enumerate(zip(sources, held))
    ]
    order = [4, 3, 8, 0, 1, 2, 9, 10, 11, 12, 6, 13, 14, 15, 16, 7, 5]
    for index in order:
        loaded[index].start()
    arrive = lambda *which: [loaded[index].wait() for index in which]
    barrier = pltpu.get_barrier_semaphore()
    greeted = [face_target(sizes, face) for face in range(6)]
    for group in (near, far):
        greeted += [device for _, device in peers(group)]
    for device in greeted:
        pl.semaphore_signal(barrier, inc=1, device_id=device, device_id_type=MESH)

    lane = lax.broadcasted_iota(jnp.int32, (16, LANES), 1)
    sub = lax.broadcasted_iota(jnp.int32, (LANES, LANES), 0)
    one = jnp.ones((LANES, LANES), bf16)
    zero = jnp.zeros((LANES, LANES), bf16)
    for part in range(total // LANES):
        node_id[part] = (sub + part * LANES).astype(jnp.int16)
        lane_id[part] = (lane + part * LANES).astype(jnp.int16)

    def column(row):
        return jnp.transpose(jnp.broadcast_to(row, (LANES, LANES)))

    arrive(4, 3, 8, 0, 1, 2, 9, 10, 11, 12)
    for block in range(edges // LANES):
        at = slice(block * LANES, (block + 1) * LANES)
        snd_col[block] = column(snd[:, at]).astype(jnp.int16)
        rcv_col[block] = column(rcv[:, at]).astype(jnp.int16)

    def node_hots(ids, start, size, count):
        rows = [
            jnp.broadcast_to(ids[:, spot : spot + LANES], (LANES, LANES)).astype(jnp.int16)
            for spot in range(start, start + size, LANES)
        ]
        return [
            jnp.concatenate([jnp.where(row == node_id[part], one, zero) for row in rows], 1)
            for part in range(count // LANES)
        ]

    def edge_hots(columns, block, first, count):
        ids = columns[block]
        return jnp.concatenate(
            [
                jnp.where(ids == jnp.concatenate([lane_id[part]] * (LANES // 16), 0), one, zero)
                for part in range(first // LANES, (first + count) // LANES)
            ],
            1,
        )

    def blocks_of(ref, start, size):
        spots = range(start // LANES, (start + size) // LANES)
        return jnp.concatenate([ref[spot] for spot in spots], 1)

    def put_blocks(ref, start, values):
        for spot in range(values.shape[1] // LANES):
            ref[start // LANES + spot] = values[:, spot * LANES : (spot + 1) * LANES]

    half = jnp.bfloat16(0.5)
    half_t = lambda weight: jnp.transpose(weight * half)
    w1 = [half_t(we1[index * width : (index + 1) * width]) for index in range(3)]
    w2, w3 = half_t(weh[0]), jnp.transpose(weh[1])
    back3, back2 = weh[1] * half, weh[0] * half
    bias = [column(0.5 * be[0:1]), column(0.5 * be[1:2]), column(be[2:3])]
    gain, shift = column(ge[...]), column(se[...])

    put_blocks(table, 0, matmul_nt(w1[1], node[...]).astype(bf16))
    put_blocks(table, nodes, matmul_nt(w1[1], ghost[...]).astype(bf16))
    put_blocks(table, total, matmul_nt(w1[2], node[...]).astype(bf16))
    spots = (total + nodes) // LANES

    agg = None
    for start, size in tiles(edges, FORWARD_TILE):
        at = pl.ds(start, size)
        rights = [jnp.transpose(edge[at])]
        rights += node_hots(snd, start, size, total) + node_hots(rcv, start, size, nodes)
        first = chain([w1[0]] + [table[spot] for spot in range(spots)], rights)
        act, slope = silu_parts(first + wide(bias[0], size))
        z1 = act.astype(bf16)
        put_blocks(z1_s, start, z1)
        put_blocks(slope1_s, start, slope)
        act, slope = silu_parts(matmul(w2, z1) + wide(bias[1], size))
        z2 = act.astype(bf16)
        put_blocks(z2_s, start, z2)
        put_blocks(slope2_s, start, slope)
        normed, inv = norm_parts(matmul(w3, z2) + wide(bias[2], size))
        put_blocks(normed_s, start, normed)
        put_blocks(inv_s, start, inv)
        new = (normed * wide(gain, size) + wide(shift, size)).astype(bf16)
        lefts = [new[:, spot : spot + LANES] for spot in range(0, size, LANES)]
        rights = [edge_hots(rcv_col, (start + spot) // LANES, 0, nodes) for spot in range(0, size, LANES)]
        term = chain(lefts, rights)
        agg = term if agg is None else agg + term

    arrive(6, 13, 14, 15, 16)
    agg = agg.astype(bf16)
    n1a, n1b = half_t(wn1[:width]), half_t(wn1[width:])
    n2, n3 = half_t(wnh[0]), jnp.transpose(wnh[1])
    first = matmul_nt(n1a, node[...]) + matmul(n1b, agg)
    act, slope1 = silu_parts(first + wide(column(0.5 * bn[0:1]), nodes))
    z1 = act.astype(bf16)
    act, slope2 = silu_parts(matmul(n2, z1) + wide(column(0.5 * bn[1:2]), nodes))
    z2 = act.astype(bf16)
    normed, inv = norm_parts(matmul(n3, z2) + wide(column(bn[2:3]), nodes))
    up = jnp.transpose(ncot[...]).astype(f32)
    gain_sum = lane_fold(up * normed)
    g3 = norm_back(up * wide(column(gn[...]), nodes), normed, inv)
    r3 = g3.astype(bf16)
    g2 = matmul(wnh[1] * half, r3) * slope2
    r2 = g2.astype(bf16)
    g1 = matmul(wnh[0] * half, r2) * slope1
    r1 = g1.astype(bf16)
    agg_grad = matmul(wn1[width:], r1).astype(bf16)
    node_part = up + matmul(wn1[:width], r1)
    node_terms = [jnp.transpose(matmul(r1, node[...])), matmul_nt(agg, r1)]
    node_terms += [matmul_nt(z1, r2), matmul_nt(z2, r3)]
    for index, term in enumerate(node_terms):
        npack[index * width : (index + 1) * width] = term * node_scale
    for pack, used in ((npack, 4 * width), (apack, 2 * width), (bpack, 3 * width)):
        if pack.shape[0] > used:
            pack[used:] = jnp.zeros((pack.shape[0] - used, width), f32)

    def row_of(folded):
        return rows_sum(jnp.transpose(folded))

    node_sums = (lane_fold(g1), lane_fold(g2), lane_fold(g3), gain_sum)
    for index, value in enumerate(node_sums):
        bpack[3 * width + 5 + index : 3 * width + 6 + index] = row_of(value) * node_scale

    pl.semaphore_wait(barrier, len(greeted))
    node_red.advance()

    arrive(7)
    small = [None] * 5
    grads = [None] * 3
    more = lambda old, new: new if old is None else old + new
    lefts = [agg_grad[:, spot : spot + LANES] for spot in range(0, nodes, LANES)]
    for start, size in tiles(edges, BACKWARD_TILE):
        at = pl.ds(start, size)
        up = jnp.transpose(ecot[at]).astype(f32)
        up = up + chain(lefts, node_hots(rcv, start, size, nodes))
        normed = blocks_of(normed_s, start, size)
        g3 = norm_back(up * wide(gain, size), normed, blocks_of(inv_s, start, size))
        r3 = g3.astype(bf16)
        g2 = matmul(back3, r3) * blocks_of(slope2_s, start, size)
        r2 = g2.astype(bf16)
        g1 = matmul(back2, r2) * blocks_of(slope1_s, start, size)
        r1 = g1.astype(bf16)
        put_blocks(r1_s, start, r1)
        grads[0] = more(grads[0], matmul(r1, edge[at]))
        grads[1] = more(grads[1], matmul_nt(blocks_of(z1_s, start, size), r2))
        grads[2] = more(grads[2], matmul_nt(blocks_of(z2_s, start, size), r3))
        for index, term in enumerate((g1, g2, g3, up * normed, up)):
            small[index] = more(small[index], lane_fold(term))
        if start == 0:
            node_red.advance()

    for index, term in enumerate((jnp.transpose(grads[0]), grads[1], grads[2])):
        bpack[index * width : (index + 1) * width] = term * edge_scale
    for index, value in enumerate(small):
        bpack[3 * width + index : 3 * width + 1 + index] = row_of(value) * edge_scale
    b_red.advance()
    node_red.advance()

    lefts = [r1_s[block] for block in range(edges // LANES)]
    by_sender = []
    for start, size in tiles(total, 2 * LANES):
        rights = [edge_hots(snd_col, block, start, size) for block in range(edges // LANES)]
        by_sender.append(chain(lefts, rights).astype(bf16))
    by_receiver = []
    for start, size in tiles(nodes, 2 * LANES):
        rights = [edge_hots(rcv_col, block, start, size) for block in range(edges // LANES)]
        by_receiver.append(chain(lefts, rights).astype(bf16))
    by_sender = jnp.concatenate(by_sender, 1)
    by_receiver = jnp.concatenate(by_receiver, 1)
    middle = matmul(by_sender[:, :nodes], node[...]) + matmul(by_sender[:, nodes:], ghost[...])
    last = matmul(by_receiver, node[...])
    apack[:width] = jnp.transpose(middle) * edge_scale
    apack[width : 2 * width] = jnp.transpose(last) * edge_scale
    a_red.advance()

    full = matmul(we1[width : 2 * width], by_sender)
    ghost_s[...] = jnp.transpose(full[:, nodes:])
    halos = []
    for face in range(6):
        rows = pl.ds(face * slots, slots)
        copy = pltpu.make_async_remote_copy(
            src_ref=ghost_s.at[rows],
            dst_ref=halo.at[rows],
            send_sem=hsend.at[face],
            recv_sem=hland.at[face],
            device_id=face_target(sizes, face),
            device_id_type=MESH,
        )
        copy.start()
        halos.append(copy)
    node_part = node_part + full[:, :nodes] + matmul(we1[2 * width :], by_receiver)
    node_o[...] = jnp.transpose(node_part)

    def edge_out(first, last):
        for block in range(first, last):
            at = pl.ds(block * LANES, LANES)
            grad = ecot[at].astype(f32) + matmul_nt(jnp.transpose(r1_s[block]), we1[:width])
            edge_o[at] = grad.astype(bf16)

    middle_block = edges // LANES // 2
    edge_out(0, middle_block)
    b_red.advance()
    node_red.advance()
    edge_out(middle_block, edges // LANES)
    a_red.advance()
    b_red.advance()
    node_red.advance()
    for copy in halos:
        copy.wait()
    arrive(5)
    spot = lax.broadcasted_iota(jnp.int32, (nodes, slots), 0)
    local = node_o[...]
    for face in range(6):
        values = halo[face * slots : (face + 1) * slots].astype(bf16)
        local = local + matmul(one_hot(spot == faces[face]), values)
    node_o[...] = local
    a_red.advance()
    b_red.advance()
    for start, target in ((0, be_o), (3, ge_o), (4, se_o), (5, bn_o), (8, gn_o)):
        start = 3 * width + start
        target[...] = bred_o[start : start + target.shape[0]]
    node_red.advance()
    a_red.advance()


def finish_kernel(node, edge, nred, bred, ared, be, ge, se, bn, gn, *refs):
    node_o, edge_o, we1_o, weh_o, be_o, ge_o, se_o, wn1_o, wnh_o, bn_o, gn_o, sems = refs
    width = node.shape[1]
    pairs = [
        (edge, edge_o),
        (node, node_o),
        (bred.at[:width], we1_o.at[:width]),
        (ared.at[: 2 * width], we1_o.at[width:]),
        (bred.at[width : 2 * width], weh_o.at[0]),
        (bred.at[2 * width : 3 * width], weh_o.at[1]),
        (nred.at[: 2 * width], wn1_o),
        (nred.at[2 * width : 3 * width], wnh_o.at[0]),
        (nred.at[3 * width : 4 * width], wnh_o.at[1]),
        (be, be_o),
        (ge, ge_o),
        (se, se_o),
        (bn, bn_o),
        (gn, gn_o),
    ]
    copies = [
        pltpu.make_async_copy(source, target, sems.at[index])
        for index, (source, target) in enumerate(pairs)
    ]
    for copy in copies:
        copy.start()
    for copy in copies:
        copy.wait()


VMEM = pl.BlockSpec(memory_space=pltpu.VMEM)
HBM = pl.BlockSpec(memory_space=pltpu.HBM)


def on_device(
    sizes,
    node_latent,
    ghost_latent,
    edge_latent,
    senders,
    receivers,
    export_rows,
    node_cotangent,
    edge_cotangent,
    w_edge_in,
    w_edge_hidden,
    b_edge,
    gain_edge,
    shift_edge,
    w_node_in,
    w_node_hidden,
    b_node,
    gain_node,
):
    f32, bf16 = jnp.float32, jnp.bfloat16
    nodes, width = node_latent.shape[3:]
    slots = ghost_latent.shape[4]
    ghosts = 6 * slots
    edges = edge_latent.shape[3]
    total = nodes + ghosts
    devices = sizes["gx"] * sizes["gy"] * sizes["gz"]
    edge_scale = float(edges * devices) ** (-0.5)
    node_scale = float(nodes * devices) ** (-0.5)

    def padded(rows, *groups):
        unit = 8
        for group in groups:
            unit *= group_size(group)
        return -(-rows // unit) * unit

    def shape(*dims, dtype=f32):
        return jax.ShapeDtypeStruct(dims, dtype)

    core, chips, near, far = stage_groups(sizes)
    nrows = padded(4 * width, core, chips)
    brows = padded(3 * width + 9, near)
    arows = padded(2 * width, near)
    reducers = [
        reducer_scratch([core, chips], far, nrows, width),
        reducer_scratch([near], far, brows, width),
        reducer_scratch([near], far, arows, width),
    ]
    operands = (
        node_latent.reshape(nodes, width),
        ghost_latent.reshape(ghosts, width),
        edge_latent.reshape(edges, width),
        senders.reshape(1, edges),
        receivers.reshape(1, edges),
        export_rows.reshape(6, 1, slots),
        node_cotangent.reshape(nodes, width),
        edge_cotangent.reshape(edges, width),
        w_edge_in,
        w_edge_hidden,
        b_edge,
        gain_edge.reshape(1, width),
        shift_edge.reshape(1, width),
        w_node_in,
        w_node_hidden,
        b_node,
        gain_node.reshape(1, width),
    )
    operands = [pltpu.with_memory_space_constraint(operand, pltpu.HBM) for operand in operands]
    counts = [len(found) for found in reducers]
    passed = pl.pallas_call(
        functools.partial(block_kernel, sizes, edge_scale, node_scale, counts),
        out_shape=(
            shape(nodes, width),
            shape(edges, width, dtype=bf16),
            shape(nrows, width),
            shape(brows, width),
            shape(arows, width),
            shape(3, width),
            shape(1, width),
            shape(1, width),
            shape(3, width),
            shape(1, width),
        ),
        in_specs=[HBM] * INPUTS,
        out_specs=(VMEM,) * 10,
        scratch_shapes=[pltpu.VMEM(operand.shape, operand.dtype) for operand in operands]
        + [
            pltpu.VMEM((total // LANES, LANES, LANES), jnp.int16),
            pltpu.VMEM((total // LANES, 16, LANES), jnp.int16),
            pltpu.VMEM((edges // LANES, LANES, LANES), jnp.int16),
            pltpu.VMEM((edges // LANES, LANES, LANES), jnp.int16),
            pltpu.VMEM(((total + nodes) // LANES, LANES, LANES), bf16),
            pltpu.VMEM((edges // LANES, LANES, LANES), bf16),
            pltpu.VMEM((edges // LANES, LANES, LANES), bf16),
            pltpu.VMEM((edges // LANES, LANES, LANES), bf16),
            pltpu.VMEM((edges // LANES, LANES, LANES), f32),
            pltpu.VMEM((edges // LANES, LANES, LANES), f32),
            pltpu.VMEM((edges // LANES, LANES, LANES), f32),
            pltpu.VMEM((edges // LANES, 1, LANES), f32),
            pltpu.VMEM((nrows, width), f32),
            pltpu.VMEM((brows, width), f32),
            pltpu.VMEM((arows, width), f32),
            pltpu.VMEM((ghosts, width), f32),
            pltpu.VMEM((ghosts, width), f32),
            pltpu.SemaphoreType.DMA((INPUTS,)),
            pltpu.SemaphoreType.DMA((6,)),
            pltpu.SemaphoreType.DMA((6,)),
        ]
        + sum(reducers, []),
        compiler_params=pltpu.CompilerParams(
            collective_id=0, has_side_effects=True, vmem_limit_bytes=32 * 1024 * 1024
        ),
        name="block_pass",
    )(*operands)

    outs = pl.pallas_call(
        finish_kernel,
        out_shape=(
            shape(nodes, width),
            shape(edges, width, dtype=bf16),
            shape(3 * width, width),
            shape(2, width, width),
            shape(3, width),
            shape(1, width),
            shape(1, width),
            shape(2 * width, width),
            shape(2, width, width),
            shape(3, width),
            shape(1, width),
        ),
        in_specs=[VMEM] * 10,
        out_specs=(HBM,) * 11,
        scratch_shapes=[pltpu.SemaphoreType.DMA((14,))],
        compiler_params=pltpu.CompilerParams(vmem_limit_bytes=4 * 1024 * 1024),
        name="finish",
    )(*passed)
    node_grad, edge_grad, we1, weh, be, ge, se, wn1, wnh, bn, gn = outs
    return (
        node_grad.reshape(node_latent.shape),
        edge_grad.reshape(edge_latent.shape),
        we1,
        weh,
        be,
        ge.reshape(width),
        se.reshape(width),
        wn1,
        wnh,
        bn,
        gn.reshape(width),
    )


def solution(mesh):
    block = P("gx", "gy", "gz")
    sizes = dict(mesh.shape)
    return jax.shard_map(
        functools.partial(on_device, sizes),
        mesh=mesh,
        in_specs=(block,) * 8 + (P(),) * 9,
        out_specs=(block,) * 2 + (P(),) * 9,
        check_vma=False,
    )
```

```python
import functools

import jax
import jax.numpy as jnp
from jax import lax
from jax.experimental import pallas as pl
from jax.experimental.pallas import tpu as pltpu
from jax.sharding import PartitionSpec as P

EPSILON = 1e-05
LANES = 128
KINDS = {"N": "near", "B": "near", "A": "near"}
PLAN = {"node": "N", "edge": "B", "scatter": "AN", "out1": "B", "out2": "A", "out3": "N", "late": "BAB", "end": "NA"}
HALO = -1
FORWARD_TILE = 768
BACKWARD_TILE = 512
MESH = pl.DeviceIdType.MESH
AXES = ("gx", "gy", "gz")


def matmul(left, right):
    return jnp.dot(left, right, preferred_element_type=jnp.float32)


def matmul_nt(left, right):
    return lax.dot_general(
        left, right, (((1,), (1,)), ((), ())), preferred_element_type=jnp.float32
    )


def contract_rows(left, right):
    return lax.dot_general(
        left, right, (((0,), (0,)), ((), ())), preferred_element_type=jnp.float32
    )


def silu_parts(half):
    th = jnp.tanh(half)
    lifted = 1.0 + th
    act = half * lifted
    return act, lifted + act * (1.0 - th)


def norm_parts(preact):
    centred = preact - jnp.mean(preact, 0, keepdims=True)
    inv_std = lax.rsqrt(jnp.mean(centred * centred, 0, keepdims=True) + EPSILON)
    return centred * inv_std, inv_std


def norm_back(scaled, normed, inv_std):
    return inv_std * (
        scaled
        - jnp.mean(scaled, 0, keepdims=True)
        - normed * jnp.mean(scaled * normed, 0, keepdims=True)
    )


def rows_sum(values):
    return jnp.sum(values, 0, keepdims=True)


def one_hot(hit):
    return jnp.where(hit, 1.0, 0.0).astype(jnp.bfloat16)


def wide(column, lanes):
    return jnp.concatenate([column] * (lanes // LANES), 1)


def lane_fold(values):
    total = values[:, :LANES]
    for start in range(LANES, values.shape[1], LANES):
        total = total + values[:, start : start + LANES]
    return total


def chain(lefts, rights):
    total = None
    for start in range(0, len(lefts), 2):
        left = jnp.concatenate(lefts[start : start + 2], 1)
        right = jnp.concatenate(rights[start : start + 2], 0)
        term = matmul(left, right)
        total = term if total is None else total + term
    return total


def stage_groups(sizes):
    pair = 2 if sizes["gz"] % 2 == 0 else 1
    core = [("gz", pair, 1)]
    chips = [("gx", sizes["gx"], 1), ("gz", sizes["gz"] // pair, pair)]
    near = core + chips
    far = [("gy", sizes["gy"], 1)]
    return core, chips, near, far


def set_groups(sizes):
    core, chips, near, far = stage_groups(sizes)
    count = sizes["gy"]
    twice = [far]
    if count % 2 == 0 and count > 2:
        twice = [[("gy", 2, 1)], [("gy", count // 2, 2)]]
    kinds = {
        "near": ([near], [far], [near]),
        "near2": ([near], twice, [near]),
        "core": ([core, chips], [far], [chips, core]),
        "core2": ([core, chips], twice, [chips, core]),
        "mix": ([near], [far], [chips, core]),
        "mix2": ([near], twice, [chips, core]),
    }
    return {name: kinds[kind] for name, kind in KINDS.items()}


def group_size(group):
    count = 1
    for _, members, _ in group:
        count *= members
    return count


def coordinate(part):
    axis, count, stride = part
    return lax.rem(lax.axis_index(axis) // stride, count)


def member(group):
    index = 0
    for part in group:
        index = index * part[1] + coordinate(part)
    return index


def peers(group):
    steps = [()]
    for part in group:
        steps = [step + (more,) for step in steps for more in range(part[1])]
    found = []
    for step in steps[1:]:
        index = 0
        device = {}
        for part, more in zip(group, step):
            axis, count, stride = part
            mine = coordinate(part)
            other = lax.rem(mine + more, count)
            index = index * count + other
            here = device.get(axis, lax.axis_index(axis))
            device[axis] = here + (other - mine) * stride
        found.append((index, device))
    return found


class Reducer:
    def __init__(self, down, lasts, up, source, out, scratch):
        self.out, self.swap = out, None
        self.scratch = list(scratch)
        self.now, self.spot, self.rows = source, 0, source.shape[0]
        self.arrived = None
        self.pending = []
        self.steps = [functools.partial(self.scatter, group) for group in down]
        self.steps += [functools.partial(self.exchange, group) for group in lasts]
        self.steps += [functools.partial(self.settle, up[0])]
        self.steps += [functools.partial(self.gather, group) for group in up[1:]]
        self.steps += [self.wait]

    def advance(self):
        self.steps.pop(0)()

    def send(self, source, target, device, spot, sems):
        copy = pltpu.make_async_remote_copy(
            src_ref=source,
            dst_ref=target,
            send_sem=sems[0].at[spot],
            recv_sem=sems[1].at[spot],
            device_id=device,
            device_id_type=MESH,
        )
        copy.start()
        self.pending.append(copy)

    def wait(self):
        for copy in self.pending:
            copy.wait()
        self.pending = []

    def fold(self):
        if self.arrived is None:
            return
        self.wait()
        landing, part, own = self.arrived
        total = own[...]
        for spot in range(self.count):
            total = total + landing[spot]
        part[...] = total
        self.now = part

    def scatter(self, group):
        self.fold()
        landing, part, *sems = self.scratch[:4]
        self.scratch = self.scratch[4:]
        piece = self.now.shape[0] // group_size(group)
        for spot, (other, device) in enumerate(peers(group)):
            rows = pl.ds(pl.multiple_of(other * piece, 8), piece)
            self.send(self.now.at[rows], landing.at[spot], device, spot, sems)
        self.count = group_size(group) - 1
        mine = member(group) * piece
        self.spot = self.spot + mine
        self.arrived = landing, part, self.now.at[pl.ds(pl.multiple_of(mine, 8), piece)]

    def swapped(self):
        self.wait()
        total = self.swap[0]
        for index in range(1, self.count):
            total = total + self.swap[index]
        return total

    def exchange(self, group):
        if self.swap is None:
            self.fold()
        else:
            total = self.swapped()
            self.now = self.scratch.pop(0)
            self.now[...] = total
        swap, *sems = self.scratch[:3]
        self.scratch = self.scratch[3:]
        mine = member(group)
        swap[mine] = self.now[...]
        for spot, (_, device) in enumerate(peers(group)):
            self.send(self.now, swap.at[mine], device, spot, sems)
        self.swap, self.count = swap, group_size(group)

    def settle(self, group):
        total = self.swapped()
        self.piece = self.now.shape[0]
        self.out[pl.ds(pl.multiple_of(self.spot, 8), self.piece)] = total
        self.gather(group)

    def gather(self, group):
        self.wait()
        sems = self.scratch[:2]
        self.scratch = self.scratch[2:]
        home = self.out.at[pl.ds(pl.multiple_of(self.spot, 8), self.piece)]
        for spot, (_, device) in enumerate(peers(group)):
            self.send(home, home, device, spot, sems)
        self.spot = self.spot - member(group) * self.piece
        self.piece = self.piece * group_size(group)


def reducer_scratch(down, lasts, up, rows, width):
    dma = pltpu.SemaphoreType.DMA
    found = []
    for group in down:
        count = group_size(group)
        rows = rows // count
        found += [pltpu.VMEM((max(count - 1, 1), rows, width), jnp.float32)]
        found += [pltpu.VMEM((rows, width), jnp.float32)]
        found += [dma((max(count - 1, 1),))] * 2
    for index, group in enumerate(lasts):
        count = group_size(group)
        if index:
            found += [pltpu.VMEM((rows, width), jnp.float32)]
        found += [pltpu.VMEM((count, rows, width), jnp.float32)] + [dma((max(count - 1, 1),))] * 2
    for group in up:
        found += [dma((max(group_size(group) - 1, 1),))] * 2
    return found


def tiles(rows, size):
    return [(start, min(size, rows - start)) for start in range(0, rows, size)]


def stagger(stages, cuts):
    waiting, running = [stages(*cut) for cut in cuts], []
    while waiting or running:
        if waiting:
            running.insert(0, waiting.pop(0))
        running = [tile for tile in running if next(tile, "done") != "done"]


def face_target(sizes, face):
    axis, side = AXES[face // 2], face % 2
    count = sizes[axis]
    step = 1 if side == 0 else count - 1
    return {axis: lax.rem(lax.axis_index(axis) + step, count)}


INPUTS = 17


def block_kernel(sizes, edge_scale, node_scale, counts, *refs):
    refs = list(refs)
    take = lambda count: [refs.pop(0) for _ in range(count)]
    sources = take(INPUTS)
    node_o, edge_o, nred_o, bred_o, ared_o, be_o, ge_o, se_o, bn_o, gn_o = take(10)
    held = take(INPUTS)
    node, ghost, edge, snd, rcv, faces, ncot, ecot, we1, weh, be, ge, se, wn1, wnh, bn, gn = held
    node_id, snd_col, rcv_col, table, z1_s, z2_s, r1_s, slope1_s, slope2_s, normed_s, inv_s = take(11)
    npack, bpack, apack, ghost_s, halo, loads, hsend, hland = take(8)
    scratch = [take(count) for count in counts]
    nodes, width = node.shape
    edges = edge.shape[0]
    ghosts = ghost.shape[0]
    slots = ghosts // 6
    total = nodes + ghosts
    bf16, f32 = jnp.bfloat16, jnp.float32
    core, chips, near, far = stage_groups(sizes)
    groups = set_groups(sizes)
    node_red = Reducer(*groups["N"], npack, nred_o, scratch[0])
    b_red = Reducer(*groups["B"], bpack, bred_o, scratch[1])
    a_red = Reducer(*groups["A"], apack, ared_o, scratch[2])

    chains = {"N": node_red, "B": b_red, "A": a_red}

    def reach(point):
        for name in PLAN.get(point, ""):
            chains[name].advance()

    loaded = [
        pltpu.make_async_copy(source, target, loads.at[index])
        for index, (source, target) in enumerate(zip(sources, held))
    ]
    order = [4, 3, 8, 0, 1, 2, 9, 10, 11, 12, 6, 13, 14, 15, 16, 7, 5]
    for index in order:
        loaded[index].start()
    arrive = lambda *which: [loaded[index].wait() for index in which]
    barrier = pltpu.get_barrier_semaphore()
    greeted = [face_target(sizes, face) for face in range(6)]
    for group in (near, far):
        greeted += [device for _, device in peers(group)]
    for device in greeted:
        pl.semaphore_signal(barrier, inc=1, device_id=device, device_id_type=MESH)

    sub = lax.broadcasted_iota(jnp.int32, (LANES, LANES), 0)
    one = jnp.ones((LANES, LANES), bf16)
    zero = jnp.zeros((LANES, LANES), bf16)
    for part in range(total // LANES):
        node_id[part] = (sub + part * LANES).astype(jnp.int16)

    def column(row):
        return jnp.transpose(jnp.broadcast_to(row, (LANES, LANES)))

    arrive(4, 3, 8, 0, 1, 2, 9, 10, 11, 12)
    for block in range(edges // LANES):
        at = slice(block * LANES, (block + 1) * LANES)
        snd_col[block] = column(snd[:, at]).astype(jnp.int16)
        rcv_col[block] = column(rcv[:, at]).astype(jnp.int16)

    def node_hots(ids, start, size, count):
        rows = [
            jnp.broadcast_to(ids[:, spot : spot + LANES], (LANES, LANES)).astype(jnp.int16)
            for spot in range(start, start + size, LANES)
        ]
        return [
            jnp.concatenate([jnp.where(row == node_id[part], one, zero) for row in rows], 1)
            for part in range(count // LANES)
        ]

    def lanes_of(part):
        spot = lax.broadcasted_iota(jnp.int32, (LANES, LANES), 1) + part * LANES
        return spot.astype(jnp.int16)

    def edge_hots(columns, block, first, count):
        ids = columns[block]
        return jnp.concatenate(
            [
                jnp.where(lanes_of(part) == ids, one, zero)
                for part in range(first // LANES, (first + count) // LANES)
            ],
            1,
        )

    more = lambda old, new: new if old is None else old + new

    def blocks_of(ref, start, size):
        spots = range(start // LANES, (start + size) // LANES)
        return jnp.concatenate([ref[spot] for spot in spots], 1)

    def put_blocks(ref, start, values):
        for spot in range(values.shape[1] // LANES):
            ref[start // LANES + spot] = values[:, spot * LANES : (spot + 1) * LANES]

    half = jnp.bfloat16(0.5)
    half_t = lambda weight: jnp.transpose(weight * half)
    w1 = [half_t(we1[index * width : (index + 1) * width]) for index in range(3)]
    w2, w3 = half_t(weh[0]), jnp.transpose(weh[1])
    back3, back2 = weh[1] * half, weh[0] * half
    bias = [column(0.5 * be[0:1]), column(0.5 * be[1:2]), column(be[2:3])]
    gain, shift = column(ge[...]), column(se[...])

    put_blocks(table, 0, (matmul_nt(w1[1], node[...]) + wide(bias[0], nodes)).astype(bf16))
    put_blocks(table, nodes, (matmul_nt(w1[1], ghost[...]) + wide(bias[0], ghosts)).astype(bf16))
    put_blocks(table, total, matmul_nt(w1[2], node[...]).astype(bf16))
    spots = (total + nodes) // LANES

    agg = [None]

    def forward(start, size):
        rights = [jnp.transpose(edge[pl.ds(start, size)])]
        rights += node_hots(snd, start, size, total) + node_hots(rcv, start, size, nodes)
        first = chain([w1[0]] + [table[spot] for spot in range(spots)], rights)
        yield
        act, slope = silu_parts(first)
        z1 = act.astype(bf16)
        put_blocks(z1_s, start, z1)
        put_blocks(slope1_s, start, slope)
        second = matmul(w2, z1)
        yield
        act, slope = silu_parts(second + wide(bias[1], size))
        z2 = act.astype(bf16)
        put_blocks(z2_s, start, z2)
        put_blocks(slope2_s, start, slope)
        third = matmul(w3, z2)
        yield
        normed, inv = norm_parts(third + wide(bias[2], size))
        put_blocks(normed_s, start, normed)
        put_blocks(inv_s, start, inv)
        new = (normed * wide(gain, size) + wide(shift, size)).astype(bf16)
        lefts = [new[:, spot : spot + LANES] for spot in range(0, size, LANES)]
        rights = [edge_hots(rcv_col, (start + spot) // LANES, 0, nodes) for spot in range(0, size, LANES)]
        agg[0] = more(agg[0], chain(lefts, rights))

    stagger(forward, tiles(edges, FORWARD_TILE))

    arrive(6, 13, 14, 15, 16)
    agg = agg[0].astype(bf16)
    n1a, n1b = half_t(wn1[:width]), half_t(wn1[width:])
    n2, n3 = half_t(wnh[0]), jnp.transpose(wnh[1])
    first = matmul_nt(n1a, node[...]) + matmul(n1b, agg)
    act, slope1 = silu_parts(first + wide(column(0.5 * bn[0:1]), nodes))
    z1 = act.astype(bf16)
    act, slope2 = silu_parts(matmul(n2, z1) + wide(column(0.5 * bn[1:2]), nodes))
    z2 = act.astype(bf16)
    normed, inv = norm_parts(matmul(n3, z2) + wide(column(bn[2:3]), nodes))
    up = jnp.transpose(ncot[...]).astype(f32)
    gain_sum = lane_fold(up * normed)
    g3 = norm_back(up * wide(column(gn[...]), nodes), normed, inv)
    r3 = g3.astype(bf16)
    g2 = matmul(wnh[1] * half, r3) * slope2
    r2 = g2.astype(bf16)
    g1 = matmul(wnh[0] * half, r2) * slope1
    r1 = g1.astype(bf16)
    agg_grad = matmul(wn1[width:], r1).astype(bf16)
    node_part = up + matmul(wn1[:width], r1)
    node_terms = [jnp.transpose(matmul(r1, node[...])), matmul_nt(agg, r1)]
    node_terms += [matmul_nt(z1, r2), matmul_nt(z2, r3)]
    for index, term in enumerate(node_terms):
        npack[index * width : (index + 1) * width] = term * node_scale
    for pack, used in ((npack, 4 * width), (apack, 2 * width), (bpack, 3 * width)):
        if pack.shape[0] > used:
            pack[used:] = jnp.zeros((pack.shape[0] - used, width), f32)

    def row_of(folded):
        return rows_sum(jnp.transpose(folded))

    node_sums = (lane_fold(g1), lane_fold(g2), lane_fold(g3), gain_sum)
    for index, value in enumerate(node_sums):
        bpack[3 * width + 5 + index : 3 * width + 6 + index] = row_of(value) * node_scale

    pl.semaphore_wait(barrier, len(greeted))
    reach("node")

    arrive(7)
    small = [None] * 5
    grads = [None] * 3
    lefts = [agg_grad[:, spot : spot + LANES] for spot in range(0, nodes, LANES)]

    def backward(start, size):
        at = pl.ds(start, size)
        up = jnp.transpose(ecot[at]).astype(f32)
        up = up + chain(lefts, node_hots(rcv, start, size, nodes))
        yield
        normed = blocks_of(normed_s, start, size)
        g3 = norm_back(up * wide(gain, size), normed, blocks_of(inv_s, start, size))
        r3 = g3.astype(bf16)
        for index, term in ((2, g3), (3, up * normed), (4, up)):
            small[index] = more(small[index], lane_fold(term))
        second = matmul(back3, r3)
        grads[2] = more(grads[2], matmul_nt(blocks_of(z2_s, start, size), r3))
        yield
        g2 = second * blocks_of(slope2_s, start, size)
        r2 = g2.astype(bf16)
        small[1] = more(small[1], lane_fold(g2))
        first = matmul(back2, r2)
        grads[1] = more(grads[1], matmul_nt(blocks_of(z1_s, start, size), r2))
        yield
        g1 = first * blocks_of(slope1_s, start, size)
        r1 = g1.astype(bf16)
        small[0] = more(small[0], lane_fold(g1))
        put_blocks(r1_s, start, r1)
        grads[0] = more(grads[0], matmul(r1, edge[at]))

    stagger(backward, tiles(edges, BACKWARD_TILE))

    for index, term in enumerate((jnp.transpose(grads[0]), grads[1], grads[2])):
        bpack[index * width : (index + 1) * width] = term * edge_scale
    for index, value in enumerate(small):
        bpack[3 * width + index : 3 * width + 1 + index] = row_of(value) * edge_scale
    reach("edge")

    lefts = [r1_s[block] for block in range(edges // LANES)]
    by_sender = []
    for start, size in tiles(total, 2 * LANES):
        rights = [edge_hots(snd_col, block, start, size) for block in range(edges // LANES)]
        by_sender.append(chain(lefts, rights).astype(bf16))
        reach("part%d" % (start // (2 * LANES)))
    by_receiver = []
    for start, size in tiles(nodes, 2 * LANES):
        rights = [edge_hots(rcv_col, block, start, size) for block in range(edges // LANES)]
        by_receiver.append(chain(lefts, rights).astype(bf16))
    by_sender = jnp.concatenate(by_sender, 1)
    by_receiver = jnp.concatenate(by_receiver, 1)
    middle = matmul(by_sender[:, :nodes], node[...]) + matmul(by_sender[:, nodes:], ghost[...])
    last = matmul(by_receiver, node[...])
    apack[:width] = jnp.transpose(middle) * edge_scale
    apack[width : 2 * width] = jnp.transpose(last) * edge_scale
    reach("scatter")

    full = matmul(we1[width : 2 * width], by_sender)
    ghost_s[...] = jnp.transpose(full[:, nodes:])
    def send_halos():
        halos = []
        for face in range(6):
            rows = pl.ds(face * slots, slots)
            copy = pltpu.make_async_remote_copy(
                src_ref=ghost_s.at[rows],
                dst_ref=halo.at[rows],
                send_sem=hsend.at[face],
                recv_sem=hland.at[face],
                device_id=face_target(sizes, face),
                device_id_type=MESH,
            )
            copy.start()
            halos.append(copy)
        return halos

    node_part = node_part + full[:, :nodes] + matmul(we1[2 * width :], by_receiver)
    node_o[...] = jnp.transpose(node_part)

    halos = send_halos() if HALO < 0 else []
    reach("halo")
    parts = 4
    for part in range(parts):
        for block in range(edges // LANES * part // parts, edges // LANES * (part + 1) // parts):
            at = pl.ds(block * LANES, LANES)
            grad = ecot[at].astype(f32) + matmul_nt(jnp.transpose(r1_s[block]), we1[:width])
            edge_o[at] = grad.astype(bf16)
        reach("out%d" % part)
        if part == HALO:
            halos = send_halos()
    for copy in halos:
        copy.wait()
    arrive(5)
    spot = lax.broadcasted_iota(jnp.int32, (nodes, slots), 0)
    local = node_o[...]
    for face in range(6):
        values = halo[face * slots : (face + 1) * slots].astype(bf16)
        local = local + matmul(one_hot(spot == faces[face]), values)
    node_o[...] = local
    reach("late")
    for start, target in ((0, be_o), (3, ge_o), (4, se_o), (5, bn_o), (8, gn_o)):
        start = 3 * width + start
        target[...] = bred_o[start : start + target.shape[0]]
    reach("end")


def finish_kernel(node, edge, nred, bred, ared, be, ge, se, bn, gn, *refs):
    node_o, edge_o, we1_o, weh_o, be_o, ge_o, se_o, wn1_o, wnh_o, bn_o, gn_o, sems = refs
    width = node.shape[1]
    pairs = [
        (edge, edge_o),
        (node, node_o),
        (bred.at[:width], we1_o.at[:width]),
        (ared.at[: 2 * width], we1_o.at[width:]),
        (bred.at[width : 2 * width], weh_o.at[0]),
        (bred.at[2 * width : 3 * width], weh_o.at[1]),
        (nred.at[: 2 * width], wn1_o),
        (nred.at[2 * width : 3 * width], wnh_o.at[0]),
        (nred.at[3 * width : 4 * width], wnh_o.at[1]),
        (be, be_o),
        (ge, ge_o),
        (se, se_o),
        (bn, bn_o),
        (gn, gn_o),
    ]
    copies = [
        pltpu.make_async_copy(source, target, sems.at[index])
        for index, (source, target) in enumerate(pairs)
    ]
    for copy in copies:
        copy.start()
    for copy in copies:
        copy.wait()


VMEM = pl.BlockSpec(memory_space=pltpu.VMEM)
HBM = pl.BlockSpec(memory_space=pltpu.HBM)


def on_device(
    sizes,
    node_latent,
    ghost_latent,
    edge_latent,
    senders,
    receivers,
    export_rows,
    node_cotangent,
    edge_cotangent,
    w_edge_in,
    w_edge_hidden,
    b_edge,
    gain_edge,
    shift_edge,
    w_node_in,
    w_node_hidden,
    b_node,
    gain_node,
):
    f32, bf16 = jnp.float32, jnp.bfloat16
    nodes, width = node_latent.shape[3:]
    slots = ghost_latent.shape[4]
    ghosts = 6 * slots
    edges = edge_latent.shape[3]
    total = nodes + ghosts
    devices = sizes["gx"] * sizes["gy"] * sizes["gz"]
    edge_scale = float(edges * devices) ** (-0.5)
    node_scale = float(nodes * devices) ** (-0.5)

    def padded(rows, *groups):
        unit = 8
        for group in groups:
            unit *= group_size(group)
        return -(-rows // unit) * unit

    def shape(*dims, dtype=f32):
        return jax.ShapeDtypeStruct(dims, dtype)

    groups = set_groups(sizes)
    nrows = padded(4 * width, *groups["N"][0])
    brows = padded(3 * width + 9, *groups["B"][0])
    arows = padded(2 * width, *groups["A"][0])
    reducers = [
        reducer_scratch(*groups["N"], nrows, width),
        reducer_scratch(*groups["B"], brows, width),
        reducer_scratch(*groups["A"], arows, width),
    ]
    operands = (
        node_latent.reshape(nodes, width),
        ghost_latent.reshape(ghosts, width),
        edge_latent.reshape(edges, width),
        senders.reshape(1, edges),
        receivers.reshape(1, edges),
        export_rows.reshape(6, 1, slots),
        node_cotangent.reshape(nodes, width),
        edge_cotangent.reshape(edges, width),
        w_edge_in,
        w_edge_hidden,
        b_edge,
        gain_edge.reshape(1, width),
        shift_edge.reshape(1, width),
        w_node_in,
        w_node_hidden,
        b_node,
        gain_node.reshape(1, width),
    )
    operands = [pltpu.with_memory_space_constraint(operand, pltpu.HBM) for operand in operands]
    counts = [len(found) for found in reducers]
    passed = pl.pallas_call(
        functools.partial(block_kernel, sizes, edge_scale, node_scale, counts),
        out_shape=(
            shape(nodes, width),
            shape(edges, width, dtype=bf16),
            shape(nrows, width),
            shape(brows, width),
            shape(arows, width),
            shape(3, width),
            shape(1, width),
            shape(1, width),
            shape(3, width),
            shape(1, width),
        ),
        in_specs=[HBM] * INPUTS,
        out_specs=(VMEM,) * 10,
        scratch_shapes=[pltpu.VMEM(operand.shape, operand.dtype) for operand in operands]
        + [
            pltpu.VMEM((total // LANES, LANES, LANES), jnp.int16),
            pltpu.VMEM((edges // LANES, LANES, LANES), jnp.int16),
            pltpu.VMEM((edges // LANES, LANES, LANES), jnp.int16),
            pltpu.VMEM(((total + nodes) // LANES, LANES, LANES), bf16),
            pltpu.VMEM((edges // LANES, LANES, LANES), bf16),
            pltpu.VMEM((edges // LANES, LANES, LANES), bf16),
            pltpu.VMEM((edges // LANES, LANES, LANES), bf16),
            pltpu.VMEM((edges // LANES, LANES, LANES), f32),
            pltpu.VMEM((edges // LANES, LANES, LANES), f32),
            pltpu.VMEM((edges // LANES, LANES, LANES), f32),
            pltpu.VMEM((edges // LANES, 1, LANES), f32),
            pltpu.VMEM((nrows, width), f32),
            pltpu.VMEM((brows, width), f32),
            pltpu.VMEM((arows, width), f32),
            pltpu.VMEM((ghosts, width), f32),
            pltpu.VMEM((ghosts, width), f32),
            pltpu.SemaphoreType.DMA((INPUTS,)),
            pltpu.SemaphoreType.DMA((6,)),
            pltpu.SemaphoreType.DMA((6,)),
        ]
        + sum(reducers, []),
        compiler_params=pltpu.CompilerParams(
            collective_id=0, has_side_effects=True, vmem_limit_bytes=32 * 1024 * 1024
        ),
        name="block_pass",
    )(*operands)

    outs = pl.pallas_call(
        finish_kernel,
        out_shape=(
            shape(nodes, width),
            shape(edges, width, dtype=bf16),
            shape(3 * width, width),
            shape(2, width, width),
            shape(3, width),
            shape(1, width),
            shape(1, width),
            shape(2 * width, width),
            shape(2, width, width),
            shape(3, width),
            shape(1, width),
        ),
        in_specs=[VMEM] * 10,
        out_specs=(HBM,) * 11,
        scratch_shapes=[pltpu.SemaphoreType.DMA((14,))],
        compiler_params=pltpu.CompilerParams(vmem_limit_bytes=4 * 1024 * 1024),
        name="finish",
    )(*passed)
    node_grad, edge_grad, we1, weh, be, ge, se, wn1, wnh, bn, gn = outs
    return (
        node_grad.reshape(node_latent.shape),
        edge_grad.reshape(edge_latent.shape),
        we1,
        weh,
        be,
        ge.reshape(width),
        se.reshape(width),
        wn1,
        wnh,
        bn,
        gn.reshape(width),
    )


def solution(mesh):
    block = P("gx", "gy", "gz")
    sizes = dict(mesh.shape)
    return jax.shard_map(
        functools.partial(on_device, sizes),
        mesh=mesh,
        in_specs=(block,) * 8 + (P(),) * 9,
        out_specs=(block,) * 2 + (P(),) * 9,
        check_vma=False,
    )
```

```python
import functools

import jax
import jax.numpy as jnp
from jax import lax
from jax.experimental import pallas as pl
from jax.experimental.pallas import tpu as pltpu
from jax.sharding import PartitionSpec as P

EPSILON = 1e-05
LANES = 128
KINDS = {"N": "core", "B": "mix", "A": "cn"}
PLAN = {"node": "N", "edge": "NB", "scatter": "A", "halo": "N", "out0": "AB", "out1": "ANB", "out2": "A", "late": "NBNB", "end": "A"}
HALO = -1
FORWARD_TILE = 768
BACKWARD_TILE = 512
MESH = pl.DeviceIdType.MESH
AXES = ("gx", "gy", "gz")


def matmul(left, right):
    return jnp.dot(left, right, preferred_element_type=jnp.float32)


def matmul_nt(left, right):
    return lax.dot_general(
        left, right, (((1,), (1,)), ((), ())), preferred_element_type=jnp.float32
    )


def contract_rows(left, right):
    return lax.dot_general(
        left, right, (((0,), (0,)), ((), ())), preferred_element_type=jnp.float32
    )


def silu_parts(half):
    th = jnp.tanh(half)
    lifted = 1.0 + th
    act = half * lifted
    return act, lifted + act * (1.0 - th)


def norm_parts(preact):
    centred = preact - jnp.mean(preact, 0, keepdims=True)
    inv_std = lax.rsqrt(jnp.mean(centred * centred, 0, keepdims=True) + EPSILON)
    return centred * inv_std, inv_std


def norm_back(scaled, normed, inv_std):
    return inv_std * (
        scaled
        - jnp.mean(scaled, 0, keepdims=True)
        - normed * jnp.mean(scaled * normed, 0, keepdims=True)
    )


def rows_sum(values):
    return jnp.sum(values, 0, keepdims=True)


def one_hot(hit):
    return jnp.where(hit, 1.0, 0.0).astype(jnp.bfloat16)


def wide(column, lanes):
    return jnp.concatenate([column] * (lanes // LANES), 1)


def lane_fold(values):
    total = values[:, :LANES]
    for start in range(LANES, values.shape[1], LANES):
        total = total + values[:, start : start + LANES]
    return total


def chain(lefts, rights):
    total = None
    for start in range(0, len(lefts), 2):
        left = jnp.concatenate(lefts[start : start + 2], 1)
        right = jnp.concatenate(rights[start : start + 2], 0)
        term = matmul(left, right)
        total = term if total is None else total + term
    return total


def stage_groups(sizes):
    pair = 2 if sizes["gz"] % 2 == 0 else 1
    core = [("gz", pair, 1)]
    chips = [("gx", sizes["gx"], 1), ("gz", sizes["gz"] // pair, pair)]
    near = core + chips
    far = [("gy", sizes["gy"], 1)]
    return core, chips, near, far


def set_groups(sizes):
    core, chips, near, far = stage_groups(sizes)
    count = sizes["gy"]
    twice = [far]
    if count % 2 == 0 and count > 2:
        twice = [[("gy", 2, 1)], [("gy", count // 2, 2)]]
    kinds = {
        "near": ([near], [far], [near]),
        "near2": ([near], twice, [near]),
        "core": ([core, chips], [far], [chips, core]),
        "core2": ([core, chips], twice, [chips, core]),
        "mix": ([near], [far], [chips, core]),
        "cn": ([core, chips], [far], [near]),
        "mix2": ([near], twice, [chips, core]),
    }
    return {name: kinds[kind] for name, kind in KINDS.items()}


def group_size(group):
    count = 1
    for _, members, _ in group:
        count *= members
    return count


def coordinate(part):
    axis, count, stride = part
    return lax.rem(lax.axis_index(axis) // stride, count)


def member(group):
    index = 0
    for part in group:
        index = index * part[1] + coordinate(part)
    return index


def hops(group, step):
    far = [min(more, part[1] - more) for part, more in zip(group, step) if part[0] != "gz" or part[2] > 1]
    return sum(far)


def peers(group):
    steps = [()]
    for part in group:
        steps = [step + (more,) for step in steps for more in range(part[1])]
    found = []
    for step in sorted(steps[1:], key=lambda step: -hops(group, step)):
        index = 0
        device = {}
        for part, more in zip(group, step):
            axis, count, stride = part
            mine = coordinate(part)
            other = lax.rem(mine + more, count)
            index = index * count + other
            here = device.get(axis, lax.axis_index(axis))
            device[axis] = here + (other - mine) * stride
        found.append((index, device))
    return found


class Reducer:
    def __init__(self, down, lasts, up, source, out, scratch):
        self.out, self.swap = out, None
        self.scratch = list(scratch)
        self.now, self.spot, self.rows = source, 0, source.shape[0]
        self.arrived = None
        self.pending = []
        self.steps = [functools.partial(self.scatter, group) for group in down]
        self.steps += [functools.partial(self.exchange, group) for group in lasts]
        self.steps += [functools.partial(self.settle, up[0])]
        self.steps += [functools.partial(self.gather, group) for group in up[1:]]
        self.steps += [self.wait]

    def advance(self):
        self.steps.pop(0)()

    def send(self, source, target, device, spot, sems):
        copy = pltpu.make_async_remote_copy(
            src_ref=source,
            dst_ref=target,
            send_sem=sems[0].at[spot],
            recv_sem=sems[1].at[spot],
            device_id=device,
            device_id_type=MESH,
        )
        copy.start()
        self.pending.append(copy)

    def wait(self):
        for copy in self.pending:
            copy.wait()
        self.pending = []

    def fold(self):
        if self.arrived is None:
            return
        self.wait()
        landing, part, own = self.arrived
        total = own[...]
        for spot in range(self.count):
            total = total + landing[spot]
        part[...] = total
        self.now = part

    def scatter(self, group):
        self.fold()
        landing, part, *sems = self.scratch[:4]
        self.scratch = self.scratch[4:]
        piece = self.now.shape[0] // group_size(group)
        for spot, (other, device) in enumerate(peers(group)):
            rows = pl.ds(pl.multiple_of(other * piece, 2), piece)
            self.send(self.now.at[rows], landing.at[spot], device, spot, sems)
        self.count = group_size(group) - 1
        mine = member(group) * piece
        self.spot = self.spot + mine
        self.arrived = landing, part, self.now.at[pl.ds(pl.multiple_of(mine, 2), piece)]

    def swapped(self):
        self.wait()
        total = self.swap[0]
        for index in range(1, self.count):
            total = total + self.swap[index]
        return total

    def exchange(self, group):
        if self.swap is None:
            self.fold()
        else:
            total = self.swapped()
            self.now = self.scratch.pop(0)
            self.now[...] = total
        swap, *sems = self.scratch[:3]
        self.scratch = self.scratch[3:]
        mine = member(group)
        swap[mine] = self.now[...]
        for spot, (_, device) in enumerate(peers(group)):
            self.send(self.now, swap.at[mine], device, spot, sems)
        self.swap, self.count = swap, group_size(group)

    def settle(self, group):
        total = self.swapped()
        self.piece = self.now.shape[0]
        self.out[pl.ds(pl.multiple_of(self.spot, 2), self.piece)] = total
        self.gather(group)

    def gather(self, group):
        self.wait()
        sems = self.scratch[:2]
        self.scratch = self.scratch[2:]
        home = self.out.at[pl.ds(pl.multiple_of(self.spot, 2), self.piece)]
        for spot, (_, device) in enumerate(peers(group)):
            self.send(home, home, device, spot, sems)
        self.spot = self.spot - member(group) * self.piece
        self.piece = self.piece * group_size(group)


def reducer_scratch(down, lasts, up, rows, width):
    dma = pltpu.SemaphoreType.DMA
    found = []
    for group in down:
        count = group_size(group)
        rows = rows // count
        found += [pltpu.VMEM((max(count - 1, 1), rows, width), jnp.float32)]
        found += [pltpu.VMEM((rows, width), jnp.float32)]
        found += [dma((max(count - 1, 1),))] * 2
    for index, group in enumerate(lasts):
        count = group_size(group)
        if index:
            found += [pltpu.VMEM((rows, width), jnp.float32)]
        found += [pltpu.VMEM((count, rows, width), jnp.float32)] + [dma((max(count - 1, 1),))] * 2
    for group in up:
        found += [dma((max(group_size(group) - 1, 1),))] * 2
    return found


def tiles(rows, size):
    return [(start, min(size, rows - start)) for start in range(0, rows, size)]


def stagger(stages, cuts):
    waiting, running = [stages(*cut) for cut in cuts], []
    while waiting or running:
        if waiting:
            running.insert(0, waiting.pop(0))
        running = [tile for tile in running if next(tile, "done") != "done"]


def face_target(sizes, face):
    axis, side = AXES[face // 2], face % 2
    count = sizes[axis]
    step = 1 if side == 0 else count - 1
    return {axis: lax.rem(lax.axis_index(axis) + step, count)}


INPUTS = 17


def block_kernel(sizes, edge_scale, node_scale, counts, *refs):
    refs = list(refs)
    take = lambda count: [refs.pop(0) for _ in range(count)]
    sources = take(INPUTS)
    node_o, edge_o, nred_o, bred_o, ared_o, be_o, ge_o, se_o, bn_o, gn_o = take(10)
    held = take(INPUTS)
    node, ghost, edge, snd, rcv, faces, ncot, ecot, we1, weh, be, ge, se, wn1, wnh, bn, gn = held
    node_id, snd_col, rcv_col, table, z1_s, z2_s, r1_s, slope1_s, slope2_s, normed_s, inv_s = take(11)
    npack, bpack, apack, ghost_s, halo, loads, hsend, hland = take(8)
    scratch = [take(count) for count in counts]
    nodes, width = node.shape
    edges = edge.shape[0]
    ghosts = ghost.shape[0]
    slots = ghosts // 6
    total = nodes + ghosts
    bf16, f32 = jnp.bfloat16, jnp.float32
    core, chips, near, far = stage_groups(sizes)
    groups = set_groups(sizes)
    node_red = Reducer(*groups["N"], npack, nred_o, scratch[0])
    b_red = Reducer(*groups["B"], bpack, bred_o, scratch[1])
    a_red = Reducer(*groups["A"], apack, ared_o, scratch[2])

    chains = {"N": node_red, "B": b_red, "A": a_red}

    def reach(point):
        for name in PLAN.get(point, ""):
            chains[name].advance()

    loaded = [
        pltpu.make_async_copy(source, target, loads.at[index])
        for index, (source, target) in enumerate(zip(sources, held))
    ]
    order = [8, 10, 0, 1, 4, 3, 2, 9, 11, 12, 6, 13, 14, 15, 16, 7, 5]
    for index in order:
        loaded[index].start()
    arrive = lambda *which: [loaded[index].wait() for index in which]
    barrier = pltpu.get_barrier_semaphore()
    greeted = [face_target(sizes, face) for face in range(6)]
    for group in (near, far):
        greeted += [device for _, device in peers(group)]
    for device in greeted:
        pl.semaphore_signal(barrier, inc=1, device_id=device, device_id_type=MESH)

    sub = lax.broadcasted_iota(jnp.int32, (LANES, LANES), 0)
    one = jnp.ones((LANES, LANES), bf16)
    zero = jnp.zeros((LANES, LANES), bf16)
    for part in range(total // LANES):
        node_id[part] = (sub + part * LANES).astype(jnp.int16)

    def column(row):
        return jnp.transpose(jnp.broadcast_to(row, (LANES, LANES)))

    arrive(8, 0, 1, 10)
    def node_hots(ids, start, size, count):
        rows = [
            jnp.broadcast_to(ids[:, spot : spot + LANES], (LANES, LANES)).astype(jnp.int16)
            for spot in range(start, start + size, LANES)
        ]
        return [
            jnp.concatenate([jnp.where(row == node_id[part], one, zero) for row in rows], 1)
            for part in range(count // LANES)
        ]

    def lanes_of(part):
        spot = lax.broadcasted_iota(jnp.int32, (LANES, LANES), 1) + part * LANES
        return spot.astype(jnp.int16)

    def edge_hots(columns, block, first, count):
        ids = columns[block]
        return jnp.concatenate(
            [
                jnp.where(lanes_of(part) == ids, one, zero)
                for part in range(first // LANES, (first + count) // LANES)
            ],
            1,
        )

    more = lambda old, new: new if old is None else old + new

    def blocks_of(ref, start, size):
        spots = range(start // LANES, (start + size) // LANES)
        return jnp.concatenate([ref[spot] for spot in spots], 1)

    def put_blocks(ref, start, values):
        for spot in range(values.shape[1] // LANES):
            ref[start // LANES + spot] = values[:, spot * LANES : (spot + 1) * LANES]

    half = jnp.bfloat16(0.5)
    half_t = lambda weight: jnp.transpose(weight * half)
    w1 = [half_t(we1[index * width : (index + 1) * width]) for index in range(3)]
    bias = [column(0.5 * be[0:1]), column(0.5 * be[1:2]), column(be[2:3])]

    put_blocks(table, 0, (matmul_nt(w1[1], node[...]) + wide(bias[0], nodes)).astype(bf16))
    put_blocks(table, nodes, (matmul_nt(w1[1], ghost[...]) + wide(bias[0], ghosts)).astype(bf16))
    put_blocks(table, total, matmul_nt(w1[2], node[...]).astype(bf16))
    spots = (total + nodes) // LANES

    arrive(4, 3, 2, 9, 11, 12)
    w2, w3 = half_t(weh[0]), jnp.transpose(weh[1])
    back3, back2 = weh[1] * half, weh[0] * half
    gain, shift = column(ge[...]), column(se[...])
    for block in range(edges // LANES):
        at = slice(block * LANES, (block + 1) * LANES)
        snd_col[block] = column(snd[:, at]).astype(jnp.int16)
        rcv_col[block] = column(rcv[:, at]).astype(jnp.int16)

    agg = [None]

    def forward(start, size):
        rights = [jnp.transpose(edge[pl.ds(start, size)])]
        rights += node_hots(snd, start, size, total) + node_hots(rcv, start, size, nodes)
        first = chain([w1[0]] + [table[spot] for spot in range(spots)], rights)
        yield
        act, slope = silu_parts(first)
        z1 = act.astype(bf16)
        put_blocks(z1_s, start, z1)
        put_blocks(slope1_s, start, slope)
        second = matmul(w2, z1)
        yield
        act, slope = silu_parts(second + wide(bias[1], size))
        z2 = act.astype(bf16)
        put_blocks(z2_s, start, z2)
        put_blocks(slope2_s, start, slope)
        third = matmul(w3, z2)
        yield
        normed, inv = norm_parts(third + wide(bias[2], size))
        put_blocks(normed_s, start, normed)
        put_blocks(inv_s, start, inv)
        new = (normed * wide(gain, size) + wide(shift, size)).astype(bf16)
        lefts = [new[:, spot : spot + LANES] for spot in range(0, size, LANES)]
        rights = [edge_hots(rcv_col, (start + spot) // LANES, 0, nodes) for spot in range(0, size, LANES)]
        agg[0] = more(agg[0], chain(lefts, rights))

    stagger(forward, tiles(edges, FORWARD_TILE))

    arrive(6, 13, 14, 15, 16)
    agg = agg[0].astype(bf16)
    n1a, n1b = half_t(wn1[:width]), half_t(wn1[width:])
    n2, n3 = half_t(wnh[0]), jnp.transpose(wnh[1])
    first = matmul_nt(n1a, node[...]) + matmul(n1b, agg)
    act, slope1 = silu_parts(first + wide(column(0.5 * bn[0:1]), nodes))
    z1 = act.astype(bf16)
    act, slope2 = silu_parts(matmul(n2, z1) + wide(column(0.5 * bn[1:2]), nodes))
    z2 = act.astype(bf16)
    normed, inv = norm_parts(matmul(n3, z2) + wide(column(bn[2:3]), nodes))
    up = jnp.transpose(ncot[...]).astype(f32)
    gain_sum = lane_fold(up * normed)
    g3 = norm_back(up * wide(column(gn[...]), nodes), normed, inv)
    r3 = g3.astype(bf16)
    g2 = matmul(wnh[1] * half, r3) * slope2
    r2 = g2.astype(bf16)
    g1 = matmul(wnh[0] * half, r2) * slope1
    r1 = g1.astype(bf16)
    agg_grad = matmul(wn1[width:], r1).astype(bf16)
    node_terms = [jnp.transpose(matmul(r1, node[...])), matmul_nt(agg, r1)]
    node_terms += [matmul_nt(z1, r2), matmul_nt(z2, r3)]
    for index, term in enumerate(node_terms):
        npack[index * width : (index + 1) * width] = term * node_scale
    for pack, used in ((npack, 4 * width), (apack, 2 * width), (bpack, 3 * width)):
        if pack.shape[0] > used:
            pack[used:] = jnp.zeros((pack.shape[0] - used, width), f32)

    pl.semaphore_wait(barrier, len(greeted))
    reach("node")

    arrive(7)
    node_part = up + matmul(wn1[:width], r1)

    def row_of(folded):
        return rows_sum(jnp.transpose(folded))

    node_sums = (lane_fold(g1), lane_fold(g2), lane_fold(g3), gain_sum)
    for index, value in enumerate(node_sums):
        bpack[3 * width + 5 + index : 3 * width + 6 + index] = row_of(value) * node_scale
    small = [None] * 5
    grads = [None] * 3
    lefts = [agg_grad[:, spot : spot + LANES] for spot in range(0, nodes, LANES)]

    def backward(start, size):
        at = pl.ds(start, size)
        up = jnp.transpose(ecot[at]).astype(f32)
        up = up + chain(lefts, node_hots(rcv, start, size, nodes))
        yield
        normed = blocks_of(normed_s, start, size)
        g3 = norm_back(up * wide(gain, size), normed, blocks_of(inv_s, start, size))
        r3 = g3.astype(bf16)
        for index, term in ((2, g3), (3, up * normed), (4, up)):
            small[index] = more(small[index], lane_fold(term))
        second = matmul(back3, r3)
        grads[2] = more(grads[2], matmul_nt(blocks_of(z2_s, start, size), r3))
        yield
        g2 = second * blocks_of(slope2_s, start, size)
        r2 = g2.astype(bf16)
        small[1] = more(small[1], lane_fold(g2))
        first = matmul(back2, r2)
        grads[1] = more(grads[1], matmul_nt(blocks_of(z1_s, start, size), r2))
        yield
        g1 = first * blocks_of(slope1_s, start, size)
        r1 = g1.astype(bf16)
        small[0] = more(small[0], lane_fold(g1))
        put_blocks(r1_s, start, r1)
        grads[0] = more(grads[0], matmul(r1, edge[at]))

    stagger(backward, tiles(edges, BACKWARD_TILE))

    for index, term in enumerate((jnp.transpose(grads[0]), grads[1], grads[2])):
        bpack[index * width : (index + 1) * width] = term * edge_scale
    for index, value in enumerate(small):
        bpack[3 * width + index : 3 * width + 1 + index] = row_of(value) * edge_scale
    reach("edge")

    lefts = [r1_s[block] for block in range(edges // LANES)]
    by_sender = []
    for start, size in tiles(total, 2 * LANES):
        rights = [edge_hots(snd_col, block, start, size) for block in range(edges // LANES)]
        by_sender.append(chain(lefts, rights).astype(bf16))
        reach("part%d" % (start // (2 * LANES)))
    by_receiver = []
    for start, size in tiles(nodes, 2 * LANES):
        rights = [edge_hots(rcv_col, block, start, size) for block in range(edges // LANES)]
        by_receiver.append(chain(lefts, rights).astype(bf16))
    by_sender = jnp.concatenate(by_sender, 1)
    by_receiver = jnp.concatenate(by_receiver, 1)
    middle = matmul(by_sender[:, :nodes], node[...]) + matmul(by_sender[:, nodes:], ghost[...])
    last = matmul(by_receiver, node[...])
    apack[:width] = jnp.transpose(middle) * edge_scale
    apack[width : 2 * width] = jnp.transpose(last) * edge_scale
    reach("scatter")

    full = matmul(we1[width : 2 * width], by_sender)
    ghost_s[...] = jnp.transpose(full[:, nodes:])
    def send_halos():
        halos = []
        for face in range(6):
            rows = pl.ds(face * slots, slots)
            copy = pltpu.make_async_remote_copy(
                src_ref=ghost_s.at[rows],
                dst_ref=halo.at[rows],
                send_sem=hsend.at[face],
                recv_sem=hland.at[face],
                device_id=face_target(sizes, face),
                device_id_type=MESH,
            )
            copy.start()
            halos.append(copy)
        return halos

    node_part = node_part + full[:, :nodes] + matmul(we1[2 * width :], by_receiver)
    node_o[...] = jnp.transpose(node_part)

    halos = send_halos() if HALO < 0 else []
    reach("halo")
    parts = 4
    for part in range(parts):
        for block in range(edges // LANES * part // parts, edges // LANES * (part + 1) // parts):
            at = pl.ds(block * LANES, LANES)
            grad = ecot[at].astype(f32) + matmul_nt(jnp.transpose(r1_s[block]), we1[:width])
            edge_o[at] = grad.astype(bf16)
        reach("out%d" % part)
        if part == HALO:
            halos = send_halos()
    for copy in halos:
        copy.wait()
    arrive(5)
    spot = lax.broadcasted_iota(jnp.int32, (nodes, slots), 0)
    local = node_o[...]
    for face in range(6):
        values = halo[face * slots : (face + 1) * slots].astype(bf16)
        local = local + matmul(one_hot(spot == faces[face]), values)
    node_o[...] = local
    reach("late")
    for start, target in ((0, be_o), (3, ge_o), (4, se_o), (5, bn_o), (8, gn_o)):
        start = 3 * width + start
        target[...] = bred_o[start : start + target.shape[0]]
    reach("end")


def finish_kernel(node, edge, nred, bred, ared, be, ge, se, bn, gn, *refs):
    node_o, edge_o, we1_o, weh_o, be_o, ge_o, se_o, wn1_o, wnh_o, bn_o, gn_o, sems = refs
    width = node.shape[1]
    pairs = [
        (edge, edge_o),
        (node, node_o),
        (bred.at[:width], we1_o.at[:width]),
        (ared.at[: 2 * width], we1_o.at[width:]),
        (bred.at[width : 2 * width], weh_o.at[0]),
        (bred.at[2 * width : 3 * width], weh_o.at[1]),
        (nred.at[: 2 * width], wn1_o),
        (nred.at[2 * width : 3 * width], wnh_o.at[0]),
        (nred.at[3 * width : 4 * width], wnh_o.at[1]),
        (be, be_o),
        (ge, ge_o),
        (se, se_o),
        (bn, bn_o),
        (gn, gn_o),
    ]
    copies = [
        pltpu.make_async_copy(source, target, sems.at[index])
        for index, (source, target) in enumerate(pairs)
    ]
    for copy in copies:
        copy.start()
    for copy in copies:
        copy.wait()


VMEM = pl.BlockSpec(memory_space=pltpu.VMEM)
HBM = pl.BlockSpec(memory_space=pltpu.HBM)


def on_device(
    sizes,
    node_latent,
    ghost_latent,
    edge_latent,
    senders,
    receivers,
    export_rows,
    node_cotangent,
    edge_cotangent,
    w_edge_in,
    w_edge_hidden,
    b_edge,
    gain_edge,
    shift_edge,
    w_node_in,
    w_node_hidden,
    b_node,
    gain_node,
):
    f32, bf16 = jnp.float32, jnp.bfloat16
    nodes, width = node_latent.shape[3:]
    slots = ghost_latent.shape[4]
    ghosts = 6 * slots
    edges = edge_latent.shape[3]
    total = nodes + ghosts
    devices = sizes["gx"] * sizes["gy"] * sizes["gz"]
    edge_scale = float(edges * devices) ** (-0.5)
    node_scale = float(nodes * devices) ** (-0.5)

    def padded(rows, *groups, unit=8):
        for group in groups:
            unit *= group_size(group)
        return -(-rows // unit) * unit

    def shape(*dims, dtype=f32):
        return jax.ShapeDtypeStruct(dims, dtype)

    groups = set_groups(sizes)
    nrows = padded(4 * width, *groups["N"][0])
    brows = padded(3 * width + 9, *groups["B"][0], unit=2)
    arows = padded(2 * width, *groups["A"][0])
    reducers = [
        reducer_scratch(*groups["N"], nrows, width),
        reducer_scratch(*groups["B"], brows, width),
        reducer_scratch(*groups["A"], arows, width),
    ]
    operands = (
        node_latent.reshape(nodes, width),
        ghost_latent.reshape(ghosts, width),
        edge_latent.reshape(edges, width),
        senders.reshape(1, edges),
        receivers.reshape(1, edges),
        export_rows.reshape(6, 1, slots),
        node_cotangent.reshape(nodes, width),
        edge_cotangent.reshape(edges, width),
        w_edge_in,
        w_edge_hidden,
        b_edge,
        gain_edge.reshape(1, width),
        shift_edge.reshape(1, width),
        w_node_in,
        w_node_hidden,
        b_node,
        gain_node.reshape(1, width),
    )
    operands = [pltpu.with_memory_space_constraint(operand, pltpu.HBM) for operand in operands]
    counts = [len(found) for found in reducers]
    passed = pl.pallas_call(
        functools.partial(block_kernel, sizes, edge_scale, node_scale, counts),
        out_shape=(
            shape(nodes, width),
            shape(edges, width, dtype=bf16),
            shape(nrows, width),
            shape(brows, width),
            shape(arows, width),
            shape(3, width),
            shape(1, width),
            shape(1, width),
            shape(3, width),
            shape(1, width),
        ),
        in_specs=[HBM] * INPUTS,
        out_specs=(VMEM,) * 10,
        scratch_shapes=[pltpu.VMEM(operand.shape, operand.dtype) for operand in operands]
        + [
            pltpu.VMEM((total // LANES, LANES, LANES), jnp.int16),
            pltpu.VMEM((edges // LANES, LANES, LANES), jnp.int16),
            pltpu.VMEM((edges // LANES, LANES, LANES), jnp.int16),
            pltpu.VMEM(((total + nodes) // LANES, LANES, LANES), bf16),
            pltpu.VMEM((edges // LANES, LANES, LANES), bf16),
            pltpu.VMEM((edges // LANES, LANES, LANES), bf16),
            pltpu.VMEM((edges // LANES, LANES, LANES), bf16),
            pltpu.VMEM((edges // LANES, LANES, LANES), f32),
            pltpu.VMEM((edges // LANES, LANES, LANES), f32),
            pltpu.VMEM((edges // LANES, LANES, LANES), f32),
            pltpu.VMEM((edges // LANES, 1, LANES), f32),
            pltpu.VMEM((nrows, width), f32),
            pltpu.VMEM((brows, width), f32),
            pltpu.VMEM((arows, width), f32),
            pltpu.VMEM((ghosts, width), f32),
            pltpu.VMEM((ghosts, width), f32),
            pltpu.SemaphoreType.DMA((INPUTS,)),
            pltpu.SemaphoreType.DMA((6,)),
            pltpu.SemaphoreType.DMA((6,)),
        ]
        + sum(reducers, []),
        compiler_params=pltpu.CompilerParams(
            collective_id=0, has_side_effects=True, vmem_limit_bytes=32 * 1024 * 1024
        ),
        name="block_pass",
    )(*operands)

    outs = pl.pallas_call(
        finish_kernel,
        out_shape=(
            shape(nodes, width),
            shape(edges, width, dtype=bf16),
            shape(3 * width, width),
            shape(2, width, width),
            shape(3, width),
            shape(1, width),
            shape(1, width),
            shape(2 * width, width),
            shape(2, width, width),
            shape(3, width),
            shape(1, width),
        ),
        in_specs=[VMEM] * 10,
        out_specs=(HBM,) * 11,
        scratch_shapes=[pltpu.SemaphoreType.DMA((14,))],
        compiler_params=pltpu.CompilerParams(vmem_limit_bytes=4 * 1024 * 1024),
        name="finish",
    )(*passed)
    node_grad, edge_grad, we1, weh, be, ge, se, wn1, wnh, bn, gn = outs
    return (
        node_grad.reshape(node_latent.shape),
        edge_grad.reshape(edge_latent.shape),
        we1,
        weh,
        be,
        ge.reshape(width),
        se.reshape(width),
        wn1,
        wnh,
        bn,
        gn.reshape(width),
    )


def solution(mesh):
    block = P("gx", "gy", "gz")
    sizes = dict(mesh.shape)
    return jax.shard_map(
        functools.partial(on_device, sizes),
        mesh=mesh,
        in_specs=(block,) * 8 + (P(),) * 9,
        out_specs=(block,) * 2 + (P(),) * 9,
        check_vma=False,
    )
```

```python
import functools

import jax
import jax.numpy as jnp
from jax import lax
from jax.experimental import pallas as pl
from jax.experimental.pallas import tpu as pltpu
from jax.sharding import PartitionSpec as P

EPSILON = 1e-05
LANES = 128
KINDS = {"N": "core", "B": "mix", "A": "cn"}
PLAN = {"node": "N", "edge": "NB", "scatter": "A", "halo": "N", "out0": "AB", "out1": "ANB", "out2": "A", "late": "NBNB", "end": "A"}
HALO = -1
FORWARD_TILE = 768
BACKWARD_TILE = 768
MESH = pl.DeviceIdType.MESH
AXES = ("gx", "gy", "gz")


def matmul(left, right):
    return jnp.dot(left, right, preferred_element_type=jnp.float32)


def matmul_nt(left, right):
    return lax.dot_general(
        left, right, (((1,), (1,)), ((), ())), preferred_element_type=jnp.float32
    )


def contract_rows(left, right):
    return lax.dot_general(
        left, right, (((0,), (0,)), ((), ())), preferred_element_type=jnp.float32
    )


def silu_parts(half):
    th = jnp.tanh(half)
    lifted = 1.0 + th
    act = half * lifted
    return act, lifted + act * (1.0 - th)


def norm_parts(preact):
    centred = preact - jnp.mean(preact, 0, keepdims=True)
    inv_std = lax.rsqrt(jnp.mean(centred * centred, 0, keepdims=True) + EPSILON)
    return centred * inv_std, inv_std


def norm_back(scaled, normed, inv_std):
    return inv_std * (
        scaled
        - jnp.mean(scaled, 0, keepdims=True)
        - normed * jnp.mean(scaled * normed, 0, keepdims=True)
    )


def rows_sum(values):
    return jnp.sum(values, 0, keepdims=True)


def one_hot(hit):
    return jnp.where(hit, 1.0, 0.0).astype(jnp.bfloat16)


def wide(column, lanes):
    return jnp.concatenate([column] * (lanes // LANES), 1)


def lane_fold(values):
    total = values[:, :LANES]
    for start in range(LANES, values.shape[1], LANES):
        total = total + values[:, start : start + LANES]
    return total


def chain(lefts, rights):
    total = None
    for start in range(0, len(lefts), 2):
        left = jnp.concatenate(lefts[start : start + 2], 1)
        right = jnp.concatenate(rights[start : start + 2], 0)
        term = matmul(left, right)
        total = term if total is None else total + term
    return total


def stage_groups(sizes):
    pair = 2 if sizes["gz"] % 2 == 0 else 1
    core = [("gz", pair, 1)]
    chips = [("gx", sizes["gx"], 1), ("gz", sizes["gz"] // pair, pair)]
    near = core + chips
    far = [("gy", sizes["gy"], 1)]
    return core, chips, near, far


def set_groups(sizes):
    core, chips, near, far = stage_groups(sizes)
    count = sizes["gy"]
    twice = [far]
    if count % 2 == 0 and count > 2:
        twice = [[("gy", 2, 1)], [("gy", count // 2, 2)]]
    kinds = {
        "near": ([near], [far], [near]),
        "near2": ([near], twice, [near]),
        "core": ([core, chips], [far], [chips, core]),
        "core2": ([core, chips], twice, [chips, core]),
        "mix": ([near], [far], [chips, core]),
        "cn": ([core, chips], [far], [near]),
        "mix2": ([near], twice, [chips, core]),
    }
    return {name: kinds[kind] for name, kind in KINDS.items()}


def group_size(group):
    count = 1
    for _, members, _ in group:
        count *= members
    return count


def coordinate(part):
    axis, count, stride = part
    return lax.rem(lax.axis_index(axis) // stride, count)


def member(group):
    index = 0
    for part in group:
        index = index * part[1] + coordinate(part)
    return index


def hops(group, step):
    far = [min(more, part[1] - more) for part, more in zip(group, step) if part[0] != "gz" or part[2] > 1]
    return sum(far)


def peers(group):
    steps = [()]
    for part in group:
        steps = [step + (more,) for step in steps for more in range(part[1])]
    found = []
    for step in sorted(steps[1:], key=lambda step: -hops(group, step)):
        index = 0
        device = {}
        for part, more in zip(group, step):
            axis, count, stride = part
            mine = coordinate(part)
            other = lax.rem(mine + more, count)
            index = index * count + other
            here = device.get(axis, lax.axis_index(axis))
            device[axis] = here + (other - mine) * stride
        found.append((index, device))
    return found


class Reducer:
    def __init__(self, down, lasts, up, source, out, scratch):
        self.out, self.swap = out, None
        self.scratch = list(scratch)
        self.now, self.spot, self.rows = source, 0, source.shape[0]
        self.arrived = None
        self.pending = []
        self.steps = [functools.partial(self.scatter, group) for group in down]
        self.steps += [functools.partial(self.exchange, group) for group in lasts]
        self.steps += [functools.partial(self.settle, up[0])]
        self.steps += [functools.partial(self.gather, group) for group in up[1:]]
        self.steps += [self.wait]

    def advance(self):
        self.steps.pop(0)()

    def send(self, source, target, device, spot, sems):
        copy = pltpu.make_async_remote_copy(
            src_ref=source,
            dst_ref=target,
            send_sem=sems[0].at[spot],
            recv_sem=sems[1].at[spot],
            device_id=device,
            device_id_type=MESH,
        )
        copy.start()
        self.pending.append(copy)

    def wait(self):
        for copy in self.pending:
            copy.wait()
        self.pending = []

    def fold(self):
        if self.arrived is None:
            return
        self.wait()
        landing, part, own = self.arrived
        total = own[...]
        for spot in range(self.count):
            total = total + landing[spot]
        part[...] = total
        self.now = part

    def scatter(self, group):
        self.fold()
        landing, part, *sems = self.scratch[:4]
        self.scratch = self.scratch[4:]
        piece = self.now.shape[0] // group_size(group)
        for spot, (other, device) in enumerate(peers(group)):
            rows = pl.ds(pl.multiple_of(other * piece, 2), piece)
            self.send(self.now.at[rows], landing.at[spot], device, spot, sems)
        self.count = group_size(group) - 1
        mine = member(group) * piece
        self.spot = self.spot + mine
        self.arrived = landing, part, self.now.at[pl.ds(pl.multiple_of(mine, 2), piece)]

    def swapped(self):
        self.wait()
        total = self.swap[0]
        for index in range(1, self.count):
            total = total + self.swap[index]
        return total

    def exchange(self, group):
        if self.swap is None:
            self.fold()
        else:
            total = self.swapped()
            self.now = self.scratch.pop(0)
            self.now[...] = total
        swap, *sems = self.scratch[:3]
        self.scratch = self.scratch[3:]
        mine = member(group)
        swap[mine] = self.now[...]
        for spot, (_, device) in enumerate(peers(group)):
            self.send(self.now, swap.at[mine], device, spot, sems)
        self.swap, self.count = swap, group_size(group)

    def settle(self, group):
        total = self.swapped()
        self.piece = self.now.shape[0]
        self.out[pl.ds(pl.multiple_of(self.spot, 2), self.piece)] = total
        self.gather(group)

    def gather(self, group):
        self.wait()
        sems = self.scratch[:2]
        self.scratch = self.scratch[2:]
        home = self.out.at[pl.ds(pl.multiple_of(self.spot, 2), self.piece)]
        for spot, (_, device) in enumerate(peers(group)):
            self.send(home, home, device, spot, sems)
        self.spot = self.spot - member(group) * self.piece
        self.piece = self.piece * group_size(group)


def reducer_scratch(down, lasts, up, rows, width):
    dma = pltpu.SemaphoreType.DMA
    found = []
    for group in down:
        count = group_size(group)
        rows = rows // count
        found += [pltpu.VMEM((max(count - 1, 1), rows, width), jnp.float32)]
        found += [pltpu.VMEM((rows, width), jnp.float32)]
        found += [dma((max(count - 1, 1),))] * 2
    for index, group in enumerate(lasts):
        count = group_size(group)
        if index:
            found += [pltpu.VMEM((rows, width), jnp.float32)]
        found += [pltpu.VMEM((count, rows, width), jnp.float32)] + [dma((max(count - 1, 1),))] * 2
    for group in up:
        found += [dma((max(group_size(group) - 1, 1),))] * 2
    return found


def tiles(rows, size):
    return [(start, min(size, rows - start)) for start in range(0, rows, size)]


def stagger(stages, cuts):
    waiting, running = [stages(*cut) for cut in cuts], []
    while waiting or running:
        if waiting:
            running.insert(0, waiting.pop(0))
        running = [tile for tile in running if next(tile, "done") != "done"]


def face_target(sizes, face):
    axis, side = AXES[face // 2], face % 2
    count = sizes[axis]
    step = 1 if side == 0 else count - 1
    return {axis: lax.rem(lax.axis_index(axis) + step, count)}


INPUTS = 17


def block_kernel(sizes, edge_scale, node_scale, counts, *refs):
    refs = list(refs)
    take = lambda count: [refs.pop(0) for _ in range(count)]
    sources = take(INPUTS)
    node_o, edge_o, nred_o, bred_o, ared_o, be_o, ge_o, se_o, bn_o, gn_o = take(10)
    held = take(INPUTS)
    node, ghost, edge, snd, rcv, faces, ncot, ecot, we1, weh, be, ge, se, wn1, wnh, bn, gn = held
    node_id, snd_col, rcv_col, table, z1_s, z2_s, r1_s, slope1_s, slope2_s, normed_s, inv_s = take(11)
    npack, bpack, apack, ghost_s, halo, loads, hsend, hland = take(8)
    scratch = [take(count) for count in counts]
    nodes, width = node.shape
    edges = edge.shape[0]
    ghosts = ghost.shape[0]
    slots = ghosts // 6
    total = nodes + ghosts
    bf16, f32 = jnp.bfloat16, jnp.float32
    core, chips, near, far = stage_groups(sizes)
    groups = set_groups(sizes)
    node_red = Reducer(*groups["N"], npack, nred_o, scratch[0])
    b_red = Reducer(*groups["B"], bpack, bred_o, scratch[1])
    a_red = Reducer(*groups["A"], apack, ared_o, scratch[2])

    chains = {"N": node_red, "B": b_red, "A": a_red}

    def reach(point):
        for name in PLAN.get(point, ""):
            chains[name].advance()

    loaded = [
        pltpu.make_async_copy(source, target, loads.at[index])
        for index, (source, target) in enumerate(zip(sources, held))
    ]
    order = [8, 10, 0, 1, 4, 3, 2, 9, 11, 12, 6, 13, 14, 15, 16, 7, 5]
    for index in order:
        loaded[index].start()
    arrive = lambda *which: [loaded[index].wait() for index in which]
    barrier = pltpu.get_barrier_semaphore()
    greeted = [face_target(sizes, face) for face in range(6)]
    for group in (near, far):
        greeted += [device for _, device in peers(group)]
    for device in greeted:
        pl.semaphore_signal(barrier, inc=1, device_id=device, device_id_type=MESH)

    sub = lax.broadcasted_iota(jnp.int32, (LANES, LANES), 0)
    one = jnp.ones((LANES, LANES), bf16)
    zero = jnp.zeros((LANES, LANES), bf16)
    for part in range(total // LANES):
        node_id[part] = (sub + part * LANES).astype(jnp.int16)

    def column(row):
        return jnp.transpose(jnp.broadcast_to(row, (LANES, LANES)))

    arrive(8, 0, 1, 10)
    def node_hots(ids, start, size, count):
        rows = [
            jnp.broadcast_to(ids[:, spot : spot + LANES], (LANES, LANES)).astype(jnp.int16)
            for spot in range(start, start + size, LANES)
        ]
        return [
            jnp.concatenate([jnp.where(row == node_id[part], one, zero) for row in rows], 1)
            for part in range(count // LANES)
        ]

    def lanes_of(part):
        spot = lax.broadcasted_iota(jnp.int32, (LANES, LANES), 1) + part * LANES
        return spot.astype(jnp.int16)

    def edge_hots(columns, block, first, count):
        ids = columns[block]
        return jnp.concatenate(
            [
                jnp.where(lanes_of(part) == ids, one, zero)
                for part in range(first // LANES, (first + count) // LANES)
            ],
            1,
        )

    more = lambda old, new: new if old is None else old + new

    def blocks_of(ref, start, size):
        spots = range(start // LANES, (start + size) // LANES)
        return jnp.concatenate([ref[spot] for spot in spots], 1)

    def put_blocks(ref, start, values):
        for spot in range(values.shape[1] // LANES):
            ref[start // LANES + spot] = values[:, spot * LANES : (spot + 1) * LANES]

    half = jnp.bfloat16(0.5)
    half_t = lambda weight: jnp.transpose(weight * half)
    w1 = [half_t(we1[index * width : (index + 1) * width]) for index in range(3)]
    bias = [column(0.5 * be[0:1]), column(0.5 * be[1:2]), column(be[2:3])]

    put_blocks(table, 0, (matmul_nt(w1[1], node[...]) + wide(bias[0], nodes)).astype(bf16))
    put_blocks(table, nodes, (matmul_nt(w1[1], ghost[...]) + wide(bias[0], ghosts)).astype(bf16))
    put_blocks(table, total, matmul_nt(w1[2], node[...]).astype(bf16))
    spots = (total + nodes) // LANES

    arrive(4, 3, 2, 9, 11, 12)
    w2, w3 = half_t(weh[0]), jnp.transpose(weh[1])
    back3, back2 = weh[1] * half, weh[0] * half
    gain, shift = column(ge[...]), column(se[...])
    for block in range(edges // LANES):
        at = slice(block * LANES, (block + 1) * LANES)
        snd_col[block] = column(snd[:, at]).astype(jnp.int16)
        rcv_col[block] = column(rcv[:, at]).astype(jnp.int16)

    agg = [None]

    def forward(start, size):
        rights = [jnp.transpose(edge[pl.ds(start, size)])]
        rights += node_hots(snd, start, size, total) + node_hots(rcv, start, size, nodes)
        first = chain([w1[0]] + [table[spot] for spot in range(spots)], rights)
        yield
        act, slope = silu_parts(first)
        z1 = act.astype(bf16)
        put_blocks(z1_s, start, z1)
        put_blocks(slope1_s, start, slope)
        second = matmul(w2, z1)
        yield
        act, slope = silu_parts(second + wide(bias[1], size))
        z2 = act.astype(bf16)
        put_blocks(z2_s, start, z2)
        put_blocks(slope2_s, start, slope)
        third = matmul(w3, z2)
        yield
        normed, inv = norm_parts(third + wide(bias[2], size))
        put_blocks(normed_s, start, normed)
        put_blocks(inv_s, start, inv)
        new = (normed * wide(gain, size) + wide(shift, size)).astype(bf16)
        lefts = [new[:, spot : spot + LANES] for spot in range(0, size, LANES)]
        rights = [edge_hots(rcv_col, (start + spot) // LANES, 0, nodes) for spot in range(0, size, LANES)]
        agg[0] = more(agg[0], chain(lefts, rights))

    stagger(forward, tiles(edges, FORWARD_TILE))

    arrive(6, 13, 14, 15, 16)
    agg = agg[0].astype(bf16)
    n1a, n1b = half_t(wn1[:width]), half_t(wn1[width:])
    n2, n3 = half_t(wnh[0]), jnp.transpose(wnh[1])
    first = matmul_nt(n1a, node[...]) + matmul(n1b, agg)
    act, slope1 = silu_parts(first + wide(column(0.5 * bn[0:1]), nodes))
    z1 = act.astype(bf16)
    act, slope2 = silu_parts(matmul(n2, z1) + wide(column(0.5 * bn[1:2]), nodes))
    z2 = act.astype(bf16)
    normed, inv = norm_parts(matmul(n3, z2) + wide(column(bn[2:3]), nodes))
    up = jnp.transpose(ncot[...]).astype(f32)
    gain_sum = lane_fold(up * normed)
    g3 = norm_back(up * wide(column(gn[...]), nodes), normed, inv)
    r3 = g3.astype(bf16)
    g2 = matmul(wnh[1] * half, r3) * slope2
    r2 = g2.astype(bf16)
    g1 = matmul(wnh[0] * half, r2) * slope1
    r1 = g1.astype(bf16)
    agg_grad = matmul(wn1[width:], r1).astype(bf16)
    node_terms = [jnp.transpose(matmul(r1, node[...])), matmul_nt(agg, r1)]
    node_terms += [matmul_nt(z1, r2), matmul_nt(z2, r3)]
    for index, term in enumerate(node_terms):
        npack[index * width : (index + 1) * width] = term * node_scale
    for pack, used in ((npack, 4 * width), (apack, 2 * width), (bpack, 3 * width)):
        if pack.shape[0] > used:
            pack[used:] = jnp.zeros((pack.shape[0] - used, width), f32)

    pl.semaphore_wait(barrier, len(greeted))
    reach("node")

    arrive(7)
    node_part = up + matmul(wn1[:width], r1)

    def row_of(folded):
        return rows_sum(jnp.transpose(folded))

    node_sums = (lane_fold(g1), lane_fold(g2), lane_fold(g3), gain_sum)
    for index, value in enumerate(node_sums):
        bpack[3 * width + 5 + index : 3 * width + 6 + index] = row_of(value) * node_scale
    small = [None] * 5
    grads = [None] * 3
    lefts = [agg_grad[:, spot : spot + LANES] for spot in range(0, nodes, LANES)]

    def backward(start, size):
        at = pl.ds(start, size)
        up = jnp.transpose(ecot[at]).astype(f32)
        up = up + chain(lefts, node_hots(rcv, start, size, nodes))
        yield
        normed = blocks_of(normed_s, start, size)
        g3 = norm_back(up * wide(gain, size), normed, blocks_of(inv_s, start, size))
        r3 = g3.astype(bf16)
        for index, term in ((2, g3), (3, up * normed), (4, up)):
            small[index] = more(small[index], lane_fold(term))
        second = matmul(back3, r3)
        grads[2] = more(grads[2], matmul_nt(blocks_of(z2_s, start, size), r3))
        yield
        g2 = second * blocks_of(slope2_s, start, size)
        r2 = g2.astype(bf16)
        small[1] = more(small[1], lane_fold(g2))
        first = matmul(back2, r2)
        grads[1] = more(grads[1], matmul_nt(blocks_of(z1_s, start, size), r2))
        yield
        g1 = first * blocks_of(slope1_s, start, size)
        r1 = g1.astype(bf16)
        small[0] = more(small[0], lane_fold(g1))
        put_blocks(r1_s, start, r1)
        grads[0] = more(grads[0], matmul(r1, edge[at]))

    stagger(backward, tiles(edges, BACKWARD_TILE))

    for index, term in enumerate((jnp.transpose(grads[0]), grads[1], grads[2])):
        bpack[index * width : (index + 1) * width] = term * edge_scale
    for index, value in enumerate(small):
        bpack[3 * width + index : 3 * width + 1 + index] = row_of(value) * edge_scale
    reach("edge")

    lefts = [r1_s[block] for block in range(edges // LANES)]
    by_sender = []
    for start, size in tiles(total, 2 * LANES):
        rights = [edge_hots(snd_col, block, start, size) for block in range(edges // LANES)]
        by_sender.append(chain(lefts, rights).astype(bf16))
        reach("part%d" % (start // (2 * LANES)))
    by_receiver = []
    for start, size in tiles(nodes, 2 * LANES):
        rights = [edge_hots(rcv_col, block, start, size) for block in range(edges // LANES)]
        by_receiver.append(chain(lefts, rights).astype(bf16))
    by_sender = jnp.concatenate(by_sender, 1)
    by_receiver = jnp.concatenate(by_receiver, 1)
    middle = matmul(by_sender[:, :nodes], node[...]) + matmul(by_sender[:, nodes:], ghost[...])
    last = matmul(by_receiver, node[...])
    apack[:width] = jnp.transpose(middle) * edge_scale
    apack[width : 2 * width] = jnp.transpose(last) * edge_scale
    reach("scatter")

    full = matmul(we1[width : 2 * width], by_sender)
    ghost_s[...] = jnp.transpose(full[:, nodes:])
    def send_halos():
        halos = []
        for face in range(6):
            rows = pl.ds(face * slots, slots)
            copy = pltpu.make_async_remote_copy(
                src_ref=ghost_s.at[rows],
                dst_ref=halo.at[rows],
                send_sem=hsend.at[face],
                recv_sem=hland.at[face],
                device_id=face_target(sizes, face),
                device_id_type=MESH,
            )
            copy.start()
            halos.append(copy)
        return halos

    node_part = node_part + full[:, :nodes] + matmul(we1[2 * width :], by_receiver)
    node_o[...] = jnp.transpose(node_part)

    halos = send_halos() if HALO < 0 else []
    reach("halo")
    parts = 4
    for part in range(parts):
        for block in range(edges // LANES * part // parts, edges // LANES * (part + 1) // parts):
            at = pl.ds(block * LANES, LANES)
            grad = ecot[at].astype(f32) + matmul_nt(jnp.transpose(r1_s[block]), we1[:width])
            edge_o[at] = grad.astype(bf16)
        reach("out%d" % part)
        if part == HALO:
            halos = send_halos()
    for copy in halos:
        copy.wait()
    arrive(5)
    spot = lax.broadcasted_iota(jnp.int32, (nodes, slots), 0)
    local = node_o[...]
    for face in range(6):
        values = halo[face * slots : (face + 1) * slots].astype(bf16)
        local = local + matmul(one_hot(spot == faces[face]), values)
    node_o[...] = local
    reach("late")
    for start, target in ((0, be_o), (3, ge_o), (4, se_o), (5, bn_o), (8, gn_o)):
        start = 3 * width + start
        target[...] = bred_o[start : start + target.shape[0]]
    reach("end")


def finish_kernel(node, edge, nred, bred, ared, be, ge, se, bn, gn, *refs):
    node_o, edge_o, we1_o, weh_o, be_o, ge_o, se_o, wn1_o, wnh_o, bn_o, gn_o, sems = refs
    width = node.shape[1]
    pairs = [
        (edge, edge_o),
        (node, node_o),
        (bred.at[:width], we1_o.at[:width]),
        (ared.at[: 2 * width], we1_o.at[width:]),
        (bred.at[width : 2 * width], weh_o.at[0]),
        (bred.at[2 * width : 3 * width], weh_o.at[1]),
        (nred.at[: 2 * width], wn1_o),
        (nred.at[2 * width : 3 * width], wnh_o.at[0]),
        (nred.at[3 * width : 4 * width], wnh_o.at[1]),
        (be, be_o),
        (ge, ge_o),
        (se, se_o),
        (bn, bn_o),
        (gn, gn_o),
    ]
    copies = [
        pltpu.make_async_copy(source, target, sems.at[index])
        for index, (source, target) in enumerate(pairs)
    ]
    for copy in copies:
        copy.start()
    for copy in copies:
        copy.wait()


VMEM = pl.BlockSpec(memory_space=pltpu.VMEM)
HBM = pl.BlockSpec(memory_space=pltpu.HBM)


def on_device(
    sizes,
    node_latent,
    ghost_latent,
    edge_latent,
    senders,
    receivers,
    export_rows,
    node_cotangent,
    edge_cotangent,
    w_edge_in,
    w_edge_hidden,
    b_edge,
    gain_edge,
    shift_edge,
    w_node_in,
    w_node_hidden,
    b_node,
    gain_node,
):
    f32, bf16 = jnp.float32, jnp.bfloat16
    nodes, width = node_latent.shape[3:]
    slots = ghost_latent.shape[4]
    ghosts = 6 * slots
    edges = edge_latent.shape[3]
    total = nodes + ghosts
    devices = sizes["gx"] * sizes["gy"] * sizes["gz"]
    edge_scale = float(edges * devices) ** (-0.5)
    node_scale = float(nodes * devices) ** (-0.5)

    def padded(rows, *groups, unit=8):
        for group in groups:
            unit *= group_size(group)
        return -(-rows // unit) * unit

    def shape(*dims, dtype=f32):
        return jax.ShapeDtypeStruct(dims, dtype)

    groups = set_groups(sizes)
    nrows = padded(4 * width, *groups["N"][0])
    brows = padded(3 * width + 9, *groups["B"][0], unit=2)
    arows = padded(2 * width, *groups["A"][0])
    reducers = [
        reducer_scratch(*groups["N"], nrows, width),
        reducer_scratch(*groups["B"], brows, width),
        reducer_scratch(*groups["A"], arows, width),
    ]
    operands = (
        node_latent.reshape(nodes, width),
        ghost_latent.reshape(ghosts, width),
        edge_latent.reshape(edges, width),
        senders.reshape(1, edges),
        receivers.reshape(1, edges),
        export_rows.reshape(6, 1, slots),
        node_cotangent.reshape(nodes, width),
        edge_cotangent.reshape(edges, width),
        w_edge_in,
        w_edge_hidden,
        b_edge,
        gain_edge.reshape(1, width),
        shift_edge.reshape(1, width),
        w_node_in,
        w_node_hidden,
        b_node,
        gain_node.reshape(1, width),
    )
    operands = [pltpu.with_memory_space_constraint(operand, pltpu.HBM) for operand in operands]
    counts = [len(found) for found in reducers]
    passed = pl.pallas_call(
        functools.partial(block_kernel, sizes, edge_scale, node_scale, counts),
        out_shape=(
            shape(nodes, width),
            shape(edges, width, dtype=bf16),
            shape(nrows, width),
            shape(brows, width),
            shape(arows, width),
            shape(3, width),
            shape(1, width),
            shape(1, width),
            shape(3, width),
            shape(1, width),
        ),
        in_specs=[HBM] * INPUTS,
        out_specs=(VMEM,) * 10,
        scratch_shapes=[pltpu.VMEM(operand.shape, operand.dtype) for operand in operands]
        + [
            pltpu.VMEM((total // LANES, LANES, LANES), jnp.int16),
            pltpu.VMEM((edges // LANES, LANES, LANES), jnp.int16),
            pltpu.VMEM((edges // LANES, LANES, LANES), jnp.int16),
            pltpu.VMEM(((total + nodes) // LANES, LANES, LANES), bf16),
            pltpu.VMEM((edges // LANES, LANES, LANES), bf16),
            pltpu.VMEM((edges // LANES, LANES, LANES), bf16),
            pltpu.VMEM((edges // LANES, LANES, LANES), bf16),
            pltpu.VMEM((edges // LANES, LANES, LANES), f32),
            pltpu.VMEM((edges // LANES, LANES, LANES), f32),
            pltpu.VMEM((edges // LANES, LANES, LANES), f32),
            pltpu.VMEM((edges // LANES, 1, LANES), f32),
            pltpu.VMEM((nrows, width), f32),
            pltpu.VMEM((brows, width), f32),
            pltpu.VMEM((arows, width), f32),
            pltpu.VMEM((ghosts, width), f32),
            pltpu.VMEM((ghosts, width), f32),
            pltpu.SemaphoreType.DMA((INPUTS,)),
            pltpu.SemaphoreType.DMA((6,)),
            pltpu.SemaphoreType.DMA((6,)),
        ]
        + sum(reducers, []),
        compiler_params=pltpu.CompilerParams(
            collective_id=0, has_side_effects=True, vmem_limit_bytes=32 * 1024 * 1024
        ),
        name="block_pass",
    )(*operands)

    outs = pl.pallas_call(
        finish_kernel,
        out_shape=(
            shape(nodes, width),
            shape(edges, width, dtype=bf16),
            shape(3 * width, width),
            shape(2, width, width),
            shape(3, width),
            shape(1, width),
            shape(1, width),
            shape(2 * width, width),
            shape(2, width, width),
            shape(3, width),
            shape(1, width),
        ),
        in_specs=[VMEM] * 10,
        out_specs=(HBM,) * 11,
        scratch_shapes=[pltpu.SemaphoreType.DMA((14,))],
        compiler_params=pltpu.CompilerParams(vmem_limit_bytes=4 * 1024 * 1024),
        name="finish",
    )(*passed)
    node_grad, edge_grad, we1, weh, be, ge, se, wn1, wnh, bn, gn = outs
    return (
        node_grad.reshape(node_latent.shape),
        edge_grad.reshape(edge_latent.shape),
        we1,
        weh,
        be,
        ge.reshape(width),
        se.reshape(width),
        wn1,
        wnh,
        bn,
        gn.reshape(width),
    )


def solution(mesh):
    block = P("gx", "gy", "gz")
    sizes = dict(mesh.shape)
    return jax.shard_map(
        functools.partial(on_device, sizes),
        mesh=mesh,
        in_specs=(block,) * 8 + (P(),) * 9,
        out_specs=(block,) * 2 + (P(),) * 9,
        check_vma=False,
    )
```
